32 devices in a mesh: groups: 2 (over x), expert: 16 (over z, y, core).
Axes of the slice: x: 2, y: 2, z: 4, core: 2. Of those that a mesh axis runs over, the one named last changes fastest.
Arguments:
- hidden_in: bfloat16 [256, 4096], P(('groups', 'expert')), parts along dimension 0, may hold values from -6 to 6
- queries: bfloat16 [256, 4096], P(('groups', 'expert')), parts along dimension 0, may hold values from -8 to 8
- decode_key_value: bfloat16 [256, 2, 256], P(('groups', 'expert')), parts along dimension 0, may hold values from -6 to 6
- local_kv: bfloat16 [1024, 2, 16, 256], P(('groups', 'expert')), parts along dimension 0, may hold values from -8 to 8
- page_table: int32 [256, 16], P(('groups', 'expert')), parts along dimension 0, may hold values from 0 to 31
- seq_blocks: int32 [256], P(('groups', 'expert')), parts along dimension 0, may hold values from 1 to 16
- prompt_kv: bfloat16 [32, 16, 2, 16, 256], P(('groups', 'expert')), parts along dimension 0, may hold values from -8 to 8
- prompt_owner: int32 [32], P('groups'), parts along dimension 0, may hold values from 0 to 15, as said below
- prompt_pages: int32 [32], P('groups'), parts along dimension 0, may hold values from 1 to 16
- norm_gain: float32 [4096], replicated, may hold values from 0.5 to 1.5
- router: bfloat16 [4096, 8], replicated, may hold values from -0.09375 to 0.09375
- w_gate: bfloat16 [16, 4096, 384], P('expert'), may hold values from -0.09375 to 0.09375
- w_up: bfloat16 [16, 4096, 384], P('expert'), may hold values from -0.09375 to 0.09375
- w_down: bfloat16 [16, 384, 4096], P('expert'), may hold values from -0.21875 to 0.21875
- route_ids: int32 [256, 8], P(('groups', 'expert')), parts along dimension 0, may hold values from 0 to 7, as said below
Outputs:
- layer_out: bfloat16 [256, 4096], P(('groups', 'expert')), parts along dimension 0
The draws below stay inside these ranges and needn't reach their ends.
There are 2 independent parts, one for each index of `groups`. The reference program is written for one: setup_inputs(seed, part) draws one part's arguments, and reference() takes and returns one part's arrays. A program takes and returns all parts, laid end to end along the dimension named above; an argument that names none is the same for every part. Nothing has to cross between parts.
Inputs may be any that keep to these rules, and one draw needn't show every extreme that they name: `prompt_owner`: each device is named by at most 2 prompts, and by exactly 2 for some of the devices. `route_ids`: each row names 8 different experts; among the rows of one device no expert is named more than 8 times, a bound that some block reaches. `page_table`: indices among the pages of the sequence's own device.
All inputs are finite; a program needn't handle non-finite values.
Results may differ from the reference program's by a relative error of at most 0.0056.
Values may be sent and summed in bfloat16 or wider, within the bound.
A program may use at most 128 MiB of HBM per device.

```python
import math
import jax
import jax.numpy as jnp
from jax import lax

D = 4096
QUERY_HEADS = 32
KEY_VALUE_HEADS = 2
HEAD_SIZE = 128
PAGE_TOKENS = 16
FW = 768
TOPK = 8
SEQ_DEV = 8
LOCAL_PAGES = 32
MAXB = 16
MAXP = 2
EXPERTS = 8
DECODE_SEQUENCES = 128
PROMPTS = 16
PROMPT_PAGES = 16
CAP = 8
N_EXPERT = 16


def draw_prompt_owner(key, part):
    owner_key, shuffle_key = jax.random.split(jax.random.fold_in(key, 11))
    owners = jax.random.permutation(owner_key, N_EXPERT)
    quarter = N_EXPERT // 4
    listed = jnp.concatenate([owners[:quarter], owners[:quarter], owners[quarter:3 * quarter]])
    shuffle = jax.random.permutation(shuffle_key, N_EXPERT)
    return listed[shuffle].astype(jnp.int32)


def draw_route_ids(key, part):
    device_keys = jax.random.split(jax.random.fold_in(key, 13), N_EXPERT)
    orders = jax.vmap(lambda single: jax.random.permutation(single, EXPERTS))(device_keys)
    window = max(TOPK, (SEQ_DEV * TOPK + CAP - 1) // CAP)
    columns = jnp.arange(SEQ_DEV * TOPK, dtype=jnp.int32) % window
    picked = jnp.take(orders, columns, axis=1)
    return picked.reshape(N_EXPERT * SEQ_DEV, TOPK).astype(jnp.int32)


def common_direction(key):
    random_signs = jax.random.randint(jax.random.fold_in(key, 101), (KEY_VALUE_HEADS * HEAD_SIZE,), 0, 2)
    return (2 * random_signs - 1).astype(jnp.float32)


def starting_noise(key, shape):
    return jnp.clip(jax.random.normal(key, shape, jnp.float32), -6.0, 6.0)


def cache_block(key, salt, leading_share):
    noise_random_key, flag_random_key, strength_random_key, value_random_key = jax.random.split(jax.random.fold_in(key, salt), 4)
    random_noise = starting_noise(noise_random_key, leading_share + (PAGE_TOKENS, KEY_VALUE_HEADS, HEAD_SIZE))
    sign_flags = jax.random.randint(flag_random_key, leading_share + (PAGE_TOKENS, KEY_VALUE_HEADS, 1), 0, 8) == 0
    blend_strength = jax.random.uniform(strength_random_key, leading_share + (PAGE_TOKENS, KEY_VALUE_HEADS, 1), jnp.float32, 5.0, 7.5)
    unit_direction = common_direction(key).reshape(KEY_VALUE_HEADS, HEAD_SIZE)
    cached_keys = jnp.where(sign_flags, 0.3 * random_noise + blend_strength * unit_direction, random_noise)
    cached_keys = jnp.clip(cached_keys, -8.0, 8.0).reshape(leading_share + (PAGE_TOKENS, KEY_VALUE_HEADS * HEAD_SIZE))
    cached_values = starting_noise(value_random_key, leading_share + (PAGE_TOKENS, KEY_VALUE_HEADS * HEAD_SIZE))
    return jnp.stack([cached_keys, cached_values], len(leading_share))


def draw_queries(key, part):
    noise_random_key, flag_random_key, strength_random_key = jax.random.split(jax.random.fold_in(key, 5), 3)
    random_noise = starting_noise(noise_random_key, (DECODE_SEQUENCES, KEY_VALUE_HEADS, QUERY_HEADS // KEY_VALUE_HEADS, HEAD_SIZE))
    sign_flags = jax.random.randint(flag_random_key, (DECODE_SEQUENCES, 1, 1, 1), 0, 4) == 0
    blend_strength = jax.random.uniform(strength_random_key, (DECODE_SEQUENCES, 1, 1, 1), jnp.float32, 2.0, 7.5)
    unit_direction = common_direction(key).reshape(1, KEY_VALUE_HEADS, 1, HEAD_SIZE)
    rows = jnp.where(sign_flags, 0.3 * random_noise + blend_strength * unit_direction, random_noise)
    return jnp.clip(rows, -8.0, 8.0).reshape(DECODE_SEQUENCES, QUERY_HEADS * HEAD_SIZE).astype(jnp.bfloat16)


def draw_local_kv(key, part):
    return cache_block(key, 7, (N_EXPERT * LOCAL_PAGES,)).astype(jnp.bfloat16)


def draw_prompt_kv(key, part):
    return cache_block(key, 8, (PROMPT_PAGES, PROMPTS)).astype(jnp.bfloat16)


def with_ends(drawn, key, smallest, high):
    place = [jax.random.randint(jax.random.fold_in(key, axis), (), 0, length) for axis, length in enumerate(drawn.shape)]
    widest = drawn.shape.index(max(drawn.shape))
    neighbour = place[:widest] + [(place[widest] + 1) % drawn.shape[widest]] + place[widest + 1:]
    return drawn.at[tuple(place)].set(smallest).at[tuple(neighbour)].set(high)


def shard_levels(rng, shape, cuts, least, high):
    gain, own = 1.0, jax.random.fold_in(rng, 6)
    for axis_at, parts in cuts:
        draws = jnp.exp(jax.random.uniform(jax.random.fold_in(own, axis_at), (parts,), jnp.float32, least / len(cuts), high / len(cuts)))
        gain = gain * jnp.repeat(draws, shape[axis_at] // parts).reshape([-1 if axis == axis_at else 1 for axis in range(len(shape))])
    return gain


def bell_draw(stream_key, extent, width, most, cuts=(), kind=jnp.bfloat16):
    values = jax.random.normal(stream_key, extent, jnp.float32) * width
    if len(cuts) > 0:
        values = shard_levels(stream_key, extent, cuts, -0.22, 0.18) * values
    return jnp.clip(values, min=-most, max=most).astype(kind)


def setup_inputs(seed: int = 0, part: int = 0) -> dict:
    splits = jax.random.split(jax.random.key(seed), 16)
    own_keys = jax.random.split(jax.random.fold_in(splits[15], part), 16)
    return {
        "hidden_in": bell_draw(own_keys[0], (DECODE_SEQUENCES, D), 1.0, 6.0, ((0, 16),)),
        "queries": draw_queries(jax.random.fold_in(jax.random.fold_in(splits[15], part), 71), part),
        "decode_key_value": bell_draw(own_keys[2], (DECODE_SEQUENCES, 2, KEY_VALUE_HEADS * HEAD_SIZE), 1.0, 6.0, ((0, 16),)),
        "local_kv": draw_local_kv(jax.random.fold_in(jax.random.fold_in(splits[15], part), 71), part),
        "page_table": with_ends(jax.random.randint(own_keys[4], (DECODE_SEQUENCES, MAXB), 0, LOCAL_PAGES), jax.random.fold_in(own_keys[4], 1), 0, LOCAL_PAGES - 1).astype(jnp.int32),
        "seq_blocks": with_ends(jax.random.randint(own_keys[5], (DECODE_SEQUENCES,), 1, MAXB + 1), jax.random.fold_in(own_keys[5], 1), 1, MAXB).astype(jnp.int32),
        "prompt_kv": draw_prompt_kv(jax.random.fold_in(jax.random.fold_in(splits[15], part), 71), part),
        "prompt_owner": draw_prompt_owner(jax.random.fold_in(jax.random.fold_in(splits[15], part), 71), part),
        "prompt_pages": with_ends(jax.random.randint(own_keys[8], (PROMPTS,), 1, PROMPT_PAGES + 1), jax.random.fold_in(own_keys[8], 1), 1, PROMPT_PAGES).astype(jnp.int32),
        "norm_gain": jnp.clip(1.0 + 0.1 * jax.random.normal(splits[9], (D,), jnp.float32), 0.5, 1.5),
        "router": bell_draw(splits[10], (D, EXPERTS), D ** -0.5, 0.09375),
        "w_gate": bell_draw(splits[11], (2 * EXPERTS, D, FW // 2), D ** -0.5, 0.09375, ((0, 16),)),
        "w_up": bell_draw(splits[12], (2 * EXPERTS, D, FW // 2), D ** -0.5, 0.09375, ((0, 16),)),
        "w_down": bell_draw(splits[13], (2 * EXPERTS, FW // 2, D), FW ** -0.5, 0.21875, ((0, 16),)),
        "route_ids": draw_route_ids(jax.random.fold_in(jax.random.fold_in(splits[15], part), 71), part),
    }


norm_eps = 1e-06
masked_score = -1e+30

def attend(rows_of_queries, rows_of_keys, rows_of_values, allowed, token_own_key, token_own_value):
    decode_tokens = rows_of_queries.shape[0]
    heads_of_queries = rows_of_queries.astype(jnp.float32).reshape(decode_tokens, KEY_VALUE_HEADS, QUERY_HEADS // KEY_VALUE_HEADS, HEAD_SIZE)
    heads_of_keys = rows_of_keys.astype(jnp.float32).reshape(decode_tokens, -1, KEY_VALUE_HEADS, HEAD_SIZE)
    heads_of_values = rows_of_values.astype(jnp.float32).reshape(decode_tokens, -1, KEY_VALUE_HEADS, HEAD_SIZE)
    scale_for_scores = 1.0 / math.sqrt(HEAD_SIZE)
    allowed_mask = allowed[:, None, None, :]
    scores = jnp.einsum('tkgd,tlkd->tkgl', heads_of_queries, heads_of_keys) * scale_for_scores
    scores = jnp.where(allowed_mask, scores, masked_score)
    token_own_score = jnp.einsum('xejp,xep->xej', heads_of_queries, token_own_key.astype(jnp.float32).reshape(decode_tokens, KEY_VALUE_HEADS, HEAD_SIZE)) * scale_for_scores
    peak = jnp.maximum(lax.optimization_barrier(jnp.max(scores, -1)), token_own_score)
    weights = jnp.where(allowed_mask, jnp.exp(scores - peak[..., None]), 0.0)
    own_weight = jnp.exp(token_own_score - peak)
    denominator = lax.optimization_barrier(jnp.sum(weights, -1)) + own_weight
    probs = lax.optimization_barrier((weights / denominator[..., None]).astype(jnp.bfloat16)).astype(jnp.float32)
    token_own_probability = lax.optimization_barrier((own_weight / denominator).astype(jnp.bfloat16)).astype(jnp.float32)
    blended_noise = jnp.einsum('tkgl,tlkd->tkgd', probs, heads_of_values)
    blended_noise = blended_noise + token_own_probability[..., None] * token_own_value.astype(jnp.float32).reshape(decode_tokens, KEY_VALUE_HEADS, 1, HEAD_SIZE)
    return blended_noise.reshape(decode_tokens, QUERY_HEADS * HEAD_SIZE).astype(jnp.bfloat16)

def reference(hidden_in, queries, decode_key_value, local_kv, page_table, seq_blocks, prompt_kv, prompt_owner, prompt_pages, norm_gain, router, w_gate, w_up, w_down, route_ids):
    devices = N_EXPERT
    experts = devices // 2
    key_value_width = KEY_VALUE_HEADS * HEAD_SIZE
    prompt_count = prompt_owner.shape[0]
    prompt_range = jnp.arange(prompt_count, dtype=jnp.int32)
    same_owner = prompt_owner[:, None] == prompt_owner[None, :]
    earlier = prompt_range[None, :] < prompt_range[:, None]
    arrival = lax.optimization_barrier(jnp.sum((same_owner & earlier).astype(jnp.int32), 1))
    matching = (prompt_owner[None, None, :] == jnp.arange(devices, dtype=jnp.int32)[:, None, None]) & (arrival[None, None, :] == jnp.arange(MAXP, dtype=jnp.int32)[None, :, None])
    chosen_prompt = lax.optimization_barrier(jnp.sum(jnp.where(matching, prompt_range[None, None, :], 0), -1)).astype(jnp.int32)
    occupied = jnp.any(matching, -1)

    def owner_attention(inputs):
        owner_index, rows_of_queries, own_kv, pool, table, blocks = inputs
        fetched = pool[table]
        old_keys = fetched[:, :, 0].reshape(SEQ_DEV, MAXB * PAGE_TOKENS, key_value_width)
        old_values = fetched[:, :, 1].reshape(SEQ_DEV, MAXB * PAGE_TOKENS, key_value_width)
        old_allowed = (jnp.arange(MAXB * PAGE_TOKENS, dtype=jnp.int32) // PAGE_TOKENS)[None, :] < blocks[:, None]
        old_out = attend(rows_of_queries, old_keys, old_values, old_allowed, own_kv[:, 0], own_kv[:, 1])
        picks = chosen_prompt[owner_index]
        fresh_pages = jnp.take(prompt_kv, picks, axis=1)
        new_keys = jnp.moveaxis(fresh_pages[:, :, 0], 1, 0).reshape(MAXP, PROMPT_PAGES * PAGE_TOKENS, key_value_width)
        new_values = jnp.moveaxis(fresh_pages[:, :, 1], 1, 0).reshape(MAXP, PROMPT_PAGES * PAGE_TOKENS, key_value_width)
        lengths = prompt_pages[picks]
        new_allowed = (jnp.arange(PROMPT_PAGES * PAGE_TOKENS, dtype=jnp.int32) // PAGE_TOKENS)[None, :] < lengths[:, None]
        new_out = attend(rows_of_queries[:MAXP], new_keys, new_values, new_allowed, own_kv[:MAXP, 0], own_kv[:MAXP, 1])
        new_count = jnp.sum(occupied[owner_index].astype(jnp.int32))
        is_new = jnp.arange(MAXP, dtype=jnp.int32) < new_count
        head_rows = jnp.where(is_new[:, None], new_out, old_out[:MAXP])
        return jnp.concatenate([head_rows, old_out[MAXP:]], 0)
    attention = lax.map(owner_attention, (jnp.arange(devices, dtype=jnp.int32), queries.reshape(devices, SEQ_DEV, QUERY_HEADS * HEAD_SIZE), decode_key_value.reshape(devices, SEQ_DEV, 2, key_value_width), local_kv.reshape(devices, LOCAL_PAGES, 2, PAGE_TOKENS, key_value_width), page_table.reshape(devices, SEQ_DEV, MAXB), seq_blocks.reshape(devices, SEQ_DEV))).reshape(DECODE_SEQUENCES, QUERY_HEADS * HEAD_SIZE)
    residual = (hidden_in.astype(jnp.float32) + attention.astype(jnp.float32)).astype(jnp.bfloat16)
    resid_wide = residual.astype(jnp.float32)
    normed = (resid_wide * lax.rsqrt(lax.optimization_barrier(jnp.mean(resid_wide * resid_wide, -1, keepdims=True)) + norm_eps) * norm_gain).astype(jnp.bfloat16)
    logits = jnp.dot(normed, router, preferred_element_type=jnp.float32)
    selected = jnp.take_along_axis(logits, route_ids, axis=1)
    gate_weights = jax.nn.softmax(selected, -1)
    assigned = SEQ_DEV * TOPK
    expert_ids = route_ids.reshape(devices, assigned)
    chosen = (expert_ids[:, :, None] == jnp.arange(experts, dtype=jnp.int32)[None, None, :]).astype(jnp.int32)
    before = jnp.cumsum(chosen, 1) - chosen
    slot_rank = lax.optimization_barrier(jnp.sum(before * chosen, 2))
    token_index = jnp.arange(devices, dtype=jnp.int32)[:, None] * SEQ_DEV + jnp.arange(assigned, dtype=jnp.int32)[None, :] // TOPK
    gate_flat = gate_weights.reshape(devices, assigned)

    def expert_step(accumulated, expert_index):
        hits = (expert_ids == expert_index)[:, None, :] & (slot_rank[:, None, :] == jnp.arange(CAP, dtype=jnp.int32)[None, :, None])
        present = jnp.any(hits, -1)
        row_token = lax.optimization_barrier(jnp.sum(jnp.where(hits, token_index[:, None, :], 0), -1)).astype(jnp.int32).reshape(-1)
        row_gate = lax.optimization_barrier(jnp.sum(jnp.where(hits, gate_flat[:, None, :], 0.0), -1)).reshape(-1)
        gathered_rows = jnp.where(present.reshape(-1)[:, None], normed[row_token], 0).astype(normed.dtype)
        expert_total = jnp.zeros((devices * CAP, D), jnp.float32)
        for half_index in range(2):
            weight_index = 2 * expert_index + half_index
            gate_proj = jnp.dot(gathered_rows, w_gate[weight_index], preferred_element_type=jnp.float32)
            up_proj = jnp.dot(gathered_rows, w_up[weight_index], preferred_element_type=jnp.float32)
            activated = (jax.nn.silu(gate_proj) * up_proj).astype(jnp.bfloat16)
            expert_total = expert_total + jnp.dot(activated, w_down[weight_index], preferred_element_type=jnp.float32)
        expert_out = lax.optimization_barrier(expert_total.astype(jnp.bfloat16)).astype(jnp.float32)
        accumulated = accumulated.at[row_token].add(expert_out * row_gate[:, None])
        return (accumulated, None)
    accumulated, _ = lax.scan(expert_step, jnp.zeros((DECODE_SEQUENCES, D), jnp.float32), jnp.arange(experts, dtype=jnp.int32))
    return (resid_wide + accumulated).astype(jnp.bfloat16)
```

```python
import functools
import math

import jax
import jax.numpy as jnp
from jax import lax
from jax.experimental import pallas as pl
from jax.experimental.pallas import tpu as pltpu
from jax.sharding import PartitionSpec as P

D = 4096
QUERY_HEADS = 32
KEY_VALUE_HEADS = 2
HEAD_SIZE = 128
PAGE_TOKENS = 16
TOPK = 8
MAXB = 16
MAXP = 2


norm_eps = 1e-06
masked_score = -1e30


def partner(x, axis, apart):
    return lax.ppermute(x, axis, [(i, i ^ 1 << apart) for i in range(lax.axis_size(axis))])


def attend(rows_of_queries, rows_of_keys, rows_of_values, allowed, token_own_key, token_own_value):
    decode_tokens = rows_of_queries.shape[0]
    heads_of_queries = rows_of_queries.reshape(
        decode_tokens, KEY_VALUE_HEADS, QUERY_HEADS // KEY_VALUE_HEADS, HEAD_SIZE
    )
    heads_of_keys = rows_of_keys.reshape(decode_tokens, -1, KEY_VALUE_HEADS, HEAD_SIZE)
    heads_of_values = rows_of_values.reshape(decode_tokens, -1, KEY_VALUE_HEADS, HEAD_SIZE)
    scale_for_scores = 1.0 / math.sqrt(HEAD_SIZE)
    allowed_mask = allowed[:, None, None, :]
    scores = (
        jnp.einsum(
            "tkgd,tlkd->tkgl", heads_of_queries, heads_of_keys, preferred_element_type=jnp.float32
        )
        * scale_for_scores
    )
    scores = jnp.where(allowed_mask, scores, masked_score)
    token_own_score = (
        jnp.einsum(
            "xejp,xep->xej",
            heads_of_queries,
            token_own_key.reshape(decode_tokens, KEY_VALUE_HEADS, HEAD_SIZE),
            preferred_element_type=jnp.float32,
        )
        * scale_for_scores
    )
    peak = jnp.maximum(jnp.max(scores, -1), token_own_score)
    weights = jnp.where(allowed_mask, jnp.exp(scores - peak[..., None]), 0.0)
    own_weight = jnp.exp(token_own_score - peak)
    denominator = jnp.sum(weights, -1) + own_weight
    probs = (weights / denominator[..., None]).astype(jnp.bfloat16)
    token_own_probability = (own_weight / denominator).astype(jnp.bfloat16)
    blended_noise = jnp.einsum(
        "tkgl,tlkd->tkgd", probs, heads_of_values, preferred_element_type=jnp.float32
    )
    blended_noise = blended_noise + token_own_probability.astype(jnp.float32)[
        ..., None
    ] * token_own_value.reshape(decode_tokens, KEY_VALUE_HEADS, 1, HEAD_SIZE).astype(jnp.float32)
    return blended_noise.reshape(decode_tokens, QUERY_HEADS * HEAD_SIZE).astype(jnp.bfloat16)


def routed(
    hidden_in,
    queries,
    decode_key_value,
    local_kv,
    page_table,
    seq_blocks,
    prompt_kv,
    prompt_owner,
    prompt_pages,
    norm_gain,
    router,
    w_gate,
    w_up,
    w_down,
    route_ids,
):
    devices = lax.axis_size("expert")
    position = lax.axis_index("expert")
    experts = devices // 2
    seq_dev = hidden_in.shape[0]
    key_value_width = KEY_VALUE_HEADS * HEAD_SIZE
    capacity = min(seq_dev, max(2, 2 * ((3 * seq_dev * TOPK + 2 * devices - 1) // (2 * devices))))
    half_cap = capacity // 2
    even_core = position % 2 == 0
    prompt_count = prompt_owner.shape[0]
    prompt_range = jnp.arange(prompt_count, dtype=jnp.int32)
    same_owner = prompt_owner[:, None] == prompt_owner[None, :]
    earlier = prompt_range[None, :] < prompt_range[:, None]
    arrival = jnp.sum((same_owner & earlier).astype(jnp.int32), 1)
    matching = (
        prompt_owner[None, None, :] == jnp.arange(devices, dtype=jnp.int32)[:, None, None]
    ) & (arrival[None, None, :] == jnp.arange(MAXP, dtype=jnp.int32)[None, :, None])
    chosen_prompt = jnp.sum(jnp.where(matching, prompt_range[None, None, :], 0), -1)
    occupied = jnp.any(matching, -1)
    own_picks = lax.dynamic_index_in_dim(chosen_prompt, position, 0, keepdims=False)
    own_occupied = lax.dynamic_index_in_dim(occupied, position, 0, keepdims=False)
    page_rows = prompt_kv[0]
    outgoing = jnp.take(page_rows, chosen_prompt.T.reshape(-1), axis=0).reshape(
        MAXP, devices, 2, PAGE_TOKENS, key_value_width
    )
    outgoing = jnp.where(occupied.T[:, :, None, None, None], outgoing, 0)
    arrived = lax.all_to_all(outgoing, "expert", split_axis=1, concat_axis=1, tiled=True)
    lengths = jnp.take(prompt_pages, own_picks)
    new_keys = arrived[:, :, 0].reshape(MAXP, devices * PAGE_TOKENS, key_value_width)
    new_values = arrived[:, :, 1].reshape(MAXP, devices * PAGE_TOKENS, key_value_width)
    new_allowed = (jnp.arange(devices * PAGE_TOKENS, dtype=jnp.int32) // PAGE_TOKENS)[
        None, :
    ] < lengths[:, None]
    fresh_rows = attend(
        queries[:MAXP],
        new_keys,
        new_values,
        new_allowed,
        decode_key_value[:MAXP, 0],
        decode_key_value[:MAXP, 1],
    )
    fetched = local_kv[page_table]
    old_keys = fetched[:, :, 0].reshape(seq_dev, MAXB * PAGE_TOKENS, key_value_width)
    old_values = fetched[:, :, 1].reshape(seq_dev, MAXB * PAGE_TOKENS, key_value_width)
    old_allowed = (jnp.arange(MAXB * PAGE_TOKENS, dtype=jnp.int32) // PAGE_TOKENS)[
        None, :
    ] < seq_blocks[:, None]
    old_out = attend(
        queries, old_keys, old_values, old_allowed, decode_key_value[:, 0], decode_key_value[:, 1]
    )
    new_count = jnp.sum(own_occupied.astype(jnp.int32))
    is_new = jnp.arange(MAXP, dtype=jnp.int32) < new_count
    attention = jnp.concatenate(
        [jnp.where(is_new[:, None], fresh_rows, old_out[:MAXP]), old_out[MAXP:]], 0
    )
    residual = (hidden_in.astype(jnp.float32) + attention.astype(jnp.float32)).astype(jnp.bfloat16)
    resid_wide = residual.astype(jnp.float32)
    normed = (
        resid_wide
        * lax.rsqrt(jnp.mean(resid_wide * resid_wide, -1, keepdims=True) + norm_eps)
        * norm_gain
    ).astype(jnp.bfloat16)
    logits = jnp.dot(normed, router, preferred_element_type=jnp.float32)
    expert_onehot = route_ids[:, :, None] == jnp.arange(experts, dtype=jnp.int32)[None, None, :]
    selected = jnp.sum(jnp.where(expert_onehot, logits[:, None, :], 0.0), -1)
    gate_weights = jax.nn.softmax(selected, -1)
    assigned = seq_dev * TOPK
    expert_ids = route_ids.reshape(assigned)
    chosen = (expert_ids[:, None] == jnp.arange(experts, dtype=jnp.int32)[None, :]).astype(
        jnp.int32
    )
    before = jnp.cumsum(chosen, 0) - chosen
    slot_rank = jnp.sum(before * chosen, 1)
    slot_index = expert_ids * capacity + slot_rank
    placing = slot_index[None, :] == jnp.arange(experts * capacity, dtype=jnp.int32)[:, None]
    selector = jnp.any(placing.reshape(experts * capacity, seq_dev, TOPK), -1).astype(jnp.bfloat16)
    gathered_rows = jnp.dot(selector, normed, preferred_element_type=jnp.float32).astype(
        jnp.bfloat16
    )
    outgoing_half = gathered_rows.reshape(devices, half_cap, D)
    own_half = lax.all_to_all(outgoing_half, "expert", split_axis=0, concat_axis=0, tiled=True)
    partner_half = partner(own_half, "expert", 0)
    received = jnp.where(
        even_core,
        jnp.concatenate([own_half, partner_half], 1),
        jnp.concatenate([partner_half, own_half], 1),
    )
    flattened = received.reshape(devices * capacity, D)
    gate_proj = jnp.dot(flattened, w_gate[0], preferred_element_type=jnp.float32)
    up_proj = jnp.dot(flattened, w_up[0], preferred_element_type=jnp.float32)
    activated = (jax.nn.silu(gate_proj) * up_proj).astype(jnp.bfloat16)
    partial_value = jnp.dot(activated, w_down[0], preferred_element_type=jnp.float32).reshape(
        devices, capacity, D
    )
    kept = jnp.where(even_core, partial_value[:, :half_cap], partial_value[:, half_cap:])
    handed = jnp.where(even_core, partial_value[:, half_cap:], partial_value[:, :half_cap])
    partner_part = partner(handed, "expert", 0)
    finished = (kept + partner_part).astype(jnp.bfloat16)
    returned = lax.all_to_all(finished, "expert", split_axis=0, concat_axis=0, tiled=True)
    expert_sum = returned.reshape(experts * capacity, D)
    picked = jnp.take(expert_sum, slot_index, axis=0).astype(jnp.float32).reshape(seq_dev, TOPK, D)
    expert_mix = jnp.sum(picked * gate_weights[:, :, None], 1)
    return (resid_wide + expert_mix).astype(jnp.bfloat16)


def layer_kernel(
    devices,
    picks,
    hidden_ref,
    q_ref,
    dkv_ref,
    kv_ref,
    table_ref,
    blocks_ref,
    pages_ref,
    lengths_ref,
    new_ref,
    gain_ref,
    router_ref,
    count_ref,
    gate_hbm,
    up_hbm,
    down_hbm,
    out_ref,
    w_gate,
    w_up,
    w_down,
    kv_send,
    kv_recv,
    attn,
    x_all,
    gates,
    part,
    core_recv,
    y_send,
    y_recv,
    z_send,
    z_recv,
    kept,
    w_sem,
    kv_ssem,
    kv_rsem,
    x_ssem,
    x_rsem,
    g_ssem,
    g_rsem,
    c_sem,
    y_sem,
    zs_sem,
    zr_sem,
):
    f32, bf16 = jnp.float32, jnp.bfloat16
    me = lax.axis_index("expert")
    lines = devices // 4
    core, row, line = lax.rem(me, 2), lax.rem(me // 2, 2), me // 4
    seqs = hidden_ref.shape[0]
    group = QUERY_HEADS // KEY_VALUE_HEADS
    scale = 1.0 / math.sqrt(HEAD_SIZE)

    def device(at_line, at_row, at_core):
        return (at_line * 2 + at_row) * 2 + at_core

    def place(at_line, at_row, at_core):
        return (at_core * 2 + at_row) * lines + at_line

    def remote(src, dst, ssem, rsem, to):
        return pltpu.make_async_remote_copy(
            src_ref=src,
            dst_ref=dst,
            send_sem=ssem,
            recv_sem=rsem,
            device_id={"expert": to},
            device_id_type=pl.DeviceIdType.MESH,
        )

    weights = [
        pltpu.make_async_copy(a.at[0], b, w_sem.at[i])
        for i, (a, b) in enumerate(((gate_hbm, w_gate), (up_hbm, w_up), (down_hbm, w_down)))
    ]
    for copy in weights:
        copy.start()

    barrier = pltpu.get_barrier_semaphore()

    def greet(k, carry):
        pl.semaphore_signal(
            barrier,
            inc=1,
            device_id={"expert": lax.rem(me + k, devices)},
            device_id_type=pl.DeviceIdType.MESH,
        )
        return carry

    lax.fori_loop(1, devices, greet, 0)

    def stage(o, carry):
        for r in range(MAXP):
            kv_send[o, r] = pages_ref[picks[o * MAXP + r]]
        return carry

    lax.fori_loop(0, devices, stage, 0)
    for r in range(MAXP):
        kv_recv[me, r] = pages_ref[picks[me * MAXP + r]]
    pl.semaphore_wait(barrier, devices - 1)

    def kv_copy(k):
        to = lax.rem(me + k, devices)
        return remote(kv_send.at[to], kv_recv.at[me], kv_ssem.at[k], kv_rsem.at[k], to)

    def kv_go(k, carry):
        kv_copy(k).start()
        return carry

    lax.fori_loop(1, devices, kv_go, 0)

    tokens = kv_ref.shape[0] * PAGE_TOKENS
    page_of = lax.broadcasted_iota(jnp.int32, (seqs, tokens), 1) // PAGE_TOKENS
    held = jnp.zeros((seqs, tokens), f32)
    for b in range(table_ref.shape[1]):
        hit = (page_of == table_ref[:, b : b + 1]) & (blocks_ref[:, 0:1] > b)
        held = held + jnp.where(hit, 1.0, 0.0)
    held = jnp.concatenate([held] * group, 0)

    def heads(h):
        rows = q_ref[...].astype(f32)
        return jnp.concatenate(
            [rows[:, (h * group + g) * HEAD_SIZE : (h * group + g + 1) * HEAD_SIZE] for g in range(group)],
            0,
        )

    def own(h, at):
        begin = at * KEY_VALUE_HEADS * HEAD_SIZE + h * HEAD_SIZE
        return jnp.concatenate([dkv_ref[:, begin : begin + HEAD_SIZE].astype(f32)] * group, 0)

    def weigh(scores, times, own_score):
        scores = jnp.where(times > 0, scores, masked_score)
        peak = jnp.maximum(jnp.max(scores, -1, keepdims=True), own_score)
        weight = times * jnp.exp(scores - peak)
        own_weight = jnp.exp(own_score - peak)
        total = jnp.sum(weight, -1, keepdims=True) + own_weight
        return (weight / total).astype(bf16), (own_weight / total).astype(bf16).astype(f32)

    def dot_t(a, b):
        return lax.dot_general(a, b, (((1,), (1,)), ((), ())), preferred_element_type=f32)

    def spread(h, mixed, old):
        for g in range(group):
            at = slice((h * group + g) * HEAD_SIZE, (h * group + g + 1) * HEAD_SIZE)
            rows = mixed[g * seqs : (g + 1) * seqs]
            if old:
                attn[:, at] = rows
            else:
                attn[:, at] = jnp.where(new_ref[:, 0:1] > 0, rows, attn[:, at])

    own_scores = []
    for h in range(KEY_VALUE_HEADS):
        at = slice(h * HEAD_SIZE, (h + 1) * HEAD_SIZE)
        queries = heads(h)
        own_score = jnp.sum(queries * own(h, 0), -1, keepdims=True) * scale
        own_scores.append(own_score)
        keys = kv_ref[:, 0, :, at].reshape(tokens, HEAD_SIZE)
        values = kv_ref[:, 1, :, at].reshape(tokens, HEAD_SIZE)
        probs, own_prob = weigh(dot_t(queries.astype(bf16), keys) * scale, held, own_score)
        mixed = jnp.dot(probs, values, preferred_element_type=f32) + own_prob * own(h, 1)
        spread(h, mixed, True)

    def kv_end(k, carry):
        kv_copy(k).wait()
        return carry

    lax.fori_loop(1, devices, kv_end, 0)

    fresh = devices * PAGE_TOKENS
    slot = lax.rem(lax.broadcasted_iota(jnp.int32, (seqs * group, 1), 0), seqs)
    ahead = lax.broadcasted_iota(jnp.int32, (seqs, fresh), 1) // PAGE_TOKENS < lengths_ref[:, 0:1]
    allowed = jnp.concatenate([jnp.where(ahead, 1.0, 0.0)] * group, 0)
    for h in range(KEY_VALUE_HEADS):
        at = slice(h * HEAD_SIZE, (h + 1) * HEAD_SIZE)
        queries = heads(h).astype(bf16)
        scores = jnp.zeros((seqs * group, fresh), f32)
        for r in range(MAXP):
            keys = kv_recv[:, r, 0, :, at].reshape(fresh, HEAD_SIZE)
            scores = jnp.where(slot == r, dot_t(queries, keys), scores)
        probs, own_prob = weigh(scores * scale, allowed, own_scores[h])
        mixed = jnp.zeros((seqs * group, HEAD_SIZE), f32)
        for r in range(MAXP):
            values = kv_recv[:, r, 1, :, at].reshape(fresh, HEAD_SIZE)
            mixed = jnp.where(
                slot == r, jnp.dot(probs, values, preferred_element_type=f32), mixed
            )
        spread(h, mixed + own_prob * own(h, 1), False)

    attention = attn[...].astype(bf16).astype(f32)
    wide = (hidden_ref[...].astype(f32) + attention).astype(bf16).astype(f32)
    attn[...] = wide
    mean = jnp.mean(wide * wide, -1, keepdims=True)
    normed = (wide * lax.rsqrt(mean + norm_eps) * gain_ref[...]).astype(bf16)
    mine = place(line, row, core)
    x_all[mine] = normed

    other_row = device(line, 1 - row, core)
    other_core = device(line, row, 1 - core)

    def pass_on(buffer, ssem, rsem, spot, at, to):
        return remote(buffer.at[spot], buffer.at[spot], ssem.at[at], rsem.at[spot], to)

    def first_hops(buffer, ssem, rsem):
        copies = [
            pass_on(buffer, ssem, rsem, mine, k, device(lax.rem(line + k, lines), row, core))
            for k in range(1, lines)
        ]
        copies.append(pass_on(buffer, ssem, rsem, mine, 0, other_row))
        copies.append(pass_on(buffer, ssem, rsem, mine, lines, other_core))
        for copy in copies:
            copy.start()
        return copies

    def arrived(buffer, ssem, rsem, spot):
        pass_on(buffer, ssem, rsem, spot, 0, other_core).wait_recv()

    pools = ((x_all, x_ssem, x_rsem), (gates, g_ssem, g_rsem))
    sent = first_hops(*pools[0])

    logits = jnp.dot(normed, router_ref[...], preferred_element_type=f32)
    times = count_ref[...]
    picked = jnp.where(times > 0, logits, masked_score)
    gate = times * jnp.exp(picked - jnp.max(picked, -1, keepdims=True))
    gate = gate / jnp.sum(gate, -1, keepdims=True)
    experts = gate.shape[1]
    gates[mine] = jnp.concatenate([gate] * (128 // experts), 1)
    sent += first_hops(*pools[1])

    for k in range(1, lines):
        spot = place(lax.rem(line + k, lines), row, core)
        for pool in pools:
            arrived(*pool, spot)
            for step, to in ((0, other_row), (1, other_core)):
                copy = pass_on(*pool, spot, lines + 2 * k - 1 + step, to)
                copy.start()
                sent.append(copy)
    for k in range(lines):
        spot = place(lax.rem(line + k, lines), 1 - row, core)
        for pool in pools:
            arrived(*pool, spot)
            copy = pass_on(*pool, spot, 3 * lines - 1 + k, other_core)
            copy.start()
            sent.append(copy)
    for at_row in range(2):
        for k in range(lines):
            for pool in pools:
                arrived(*pool, place(k, at_row, 1 - core))

    weights[0].wait()
    weights[1].wait()
    total = devices * seqs
    hidden = w_gate.shape[1]
    step = min(512, D)

    def project(i, carry):
        at = pl.ds(pl.multiple_of(i * step, step), step)
        x = x_all[:, :, at].reshape(total, step)
        return (
            carry[0] + jnp.dot(x, w_gate[at, :], preferred_element_type=f32),
            carry[1] + jnp.dot(x, w_up[at, :], preferred_element_type=f32),
        )

    zeros = jnp.zeros((total, hidden), f32)
    gate_proj, up_proj = lax.fori_loop(0, D // step, project, (zeros, zeros))
    lanes = lax.broadcasted_iota(jnp.int32, (total, 128), 1)
    scaled = jnp.sum(
        jnp.where(lanes == me // 2, gates[...].reshape(total, 128), 0.0), -1, keepdims=True
    )
    activated = (gate_proj / (1.0 + jnp.exp(-gate_proj)) * up_proj * scaled).astype(bf16)

    weights[2].wait()
    chunks = c_sem.shape[1]
    width = D // chunks

    def cut(i):
        return slice(i * width, (i + 1) * width)

    def core_copy(i):
        return remote(
            part.at[1 - core, :, :, :, cut(i)],
            core_recv.at[:, :, :, cut(i)],
            c_sem.at[0, i],
            c_sem.at[1, i],
            other_core,
        )

    def row_copy(i):
        return remote(
            y_send.at[:, :, cut(i)],
            y_recv.at[:, :, cut(i)],
            y_sem.at[0, i],
            y_sem.at[1, i],
            other_row,
        )

    def line_copy(i, k):
        to = lax.rem(line + k, lines)
        return remote(
            z_send.at[k, :, cut(i)],
            z_recv.at[k, :, cut(i)],
            zs_sem.at[k, i],
            zr_sem.at[k, i],
            device(to, row, core),
        )

    for i in range(chunks):
        rows = jnp.dot(activated, w_down[:, cut(i)], preferred_element_type=f32)
        part[:, :, :, :, cut(i)] = rows.astype(bf16).reshape(2, 2, lines, seqs, width)
        core_copy(i).start()
    for i in range(chunks):
        core_copy(i).wait()
        y_send[:, :, cut(i)] = (
            part[core, 1 - row, :, :, cut(i)].astype(f32)
            + core_recv[1 - row, :, :, cut(i)].astype(f32)
        ).astype(bf16)
        row_copy(i).start()
    for i in range(chunks):
        row_copy(i).wait()

        def summed(at_line):
            return (
                part[core, row, at_line, :, cut(i)].astype(f32)
                + core_recv[row, at_line, :, cut(i)].astype(f32)
                + y_recv[at_line, :, cut(i)].astype(f32)
            )

        for k in range(1, lines):
            z_send[k, :, cut(i)] = summed(lax.rem(line + k, lines)).astype(bf16)
            line_copy(i, k).start()
        kept[:, cut(i)] = attn[:, cut(i)] + summed(line)
    for i in range(chunks):
        answer = kept[:, cut(i)]
        for k in range(1, lines):
            line_copy(i, k).wait()
            answer = answer + z_recv[k, :, cut(i)].astype(f32)
        out_ref[:, cut(i)] = answer.astype(bf16)
    for copy in sent:
        copy.wait_send()


def dense(
    hidden_in,
    queries,
    decode_key_value,
    local_kv,
    page_table,
    seq_blocks,
    prompt_kv,
    prompt_owner,
    prompt_pages,
    norm_gain,
    router,
    w_gate,
    w_up,
    w_down,
    route_ids,
):
    devices = lax.axis_size("expert")
    position = lax.axis_index("expert")
    experts = router.shape[1]
    seqs = hidden_in.shape[0]
    hidden = w_gate.shape[2]
    lines = devices // 4
    bf16, f32 = jnp.bfloat16, jnp.float32
    prompt_range = jnp.arange(prompt_owner.shape[0], dtype=jnp.int32)
    same_owner = prompt_owner[:, None] == prompt_owner[None, :]
    earlier = prompt_range[None, :] < prompt_range[:, None]
    arrival = jnp.sum((same_owner & earlier).astype(jnp.int32), 1)
    pair = prompt_owner * MAXP + arrival
    slots = jnp.arange(devices * MAXP, dtype=jnp.int32)
    picks = jnp.sum(jnp.where(pair[None, :] == slots[:, None], prompt_range[None, :], 0), 1)
    slot = jnp.arange(seqs, dtype=jnp.int32)
    here = (prompt_owner[None, :] == position) & (arrival[None, :] == slot[:, None])
    lengths = jnp.sum(jnp.where(here, prompt_pages[None, :], 0), 1, keepdims=True)
    is_new = jnp.any(here, 1, keepdims=True).astype(jnp.int32)
    ids = jnp.arange(experts, dtype=jnp.int32)
    counts = jnp.sum((route_ids[:, :, None] == ids[None, None, :]).astype(f32), 1)
    chunks = 4
    smem = pl.BlockSpec(memory_space=pltpu.SMEM)
    vmem = pl.BlockSpec(memory_space=pltpu.VMEM)
    hbm = pl.BlockSpec(memory_space=pl.ANY)
    dma = pltpu.SemaphoreType.DMA
    page = (MAXP, 2, PAGE_TOKENS, KEY_VALUE_HEADS * HEAD_SIZE)
    return pl.pallas_call(
        functools.partial(layer_kernel, devices),
        out_shape=jax.ShapeDtypeStruct((seqs, D), bf16),
        in_specs=[smem] + [vmem] * 12 + [hbm] * 3,
        out_specs=vmem,
        scratch_shapes=[
            pltpu.VMEM((D, hidden), bf16),
            pltpu.VMEM((D, hidden), bf16),
            pltpu.VMEM((hidden, D), bf16),
            pltpu.VMEM((devices,) + page, bf16),
            pltpu.VMEM((devices,) + page, bf16),
            pltpu.VMEM((seqs, D), f32),
            pltpu.VMEM((devices, seqs, D), bf16),
            pltpu.VMEM((devices, seqs, 128), f32),
            pltpu.VMEM((2, 2, lines, seqs, D), bf16),
            pltpu.VMEM((2, lines, seqs, D), bf16),
            pltpu.VMEM((lines, seqs, D), bf16),
            pltpu.VMEM((lines, seqs, D), bf16),
            pltpu.VMEM((lines, seqs, D), bf16),
            pltpu.VMEM((lines, seqs, D), bf16),
            pltpu.VMEM((seqs, D), f32),
            dma((3,)),
            dma((devices,)),
            dma((devices,)),
            dma((4 * lines,)),
            dma((devices,)),
            dma((4 * lines,)),
            dma((devices,)),
            dma((2, chunks)),
            dma((2, chunks)),
            dma((lines, chunks)),
            dma((lines, chunks)),
        ],
        compiler_params=pltpu.CompilerParams(
            collective_id=0, has_side_effects=True, vmem_limit_bytes=48 << 20
        ),
    )(
        picks,
        hidden_in,
        queries,
        decode_key_value.reshape(seqs, -1),
        local_kv,
        page_table,
        seq_blocks[:, None],
        prompt_kv[0],
        lengths,
        is_new,
        norm_gain[None, :],
        router,
        counts,
        w_gate,
        w_up,
        w_down,
    )


def local(*arrays):
    devices = lax.axis_size("expert")
    experts = arrays[10].shape[1]
    if experts == TOPK and devices == 2 * experts and devices % 4 == 0:
        return dense(*arrays)
    return routed(*arrays)


def solution(mesh):
    return jax.shard_map(
        local,
        mesh=mesh,
        in_specs=(
            P(("groups", "expert"), None),
            P(("groups", "expert"), None),
            P(("groups", "expert"), None, None),
            P(("groups", "expert"), None, None, None),
            P(("groups", "expert"), None),
            P(("groups", "expert")),
            P(("groups", "expert"), None, None, None, None),
            P("groups"),
            P("groups"),
            P(),
            P(),
            P("expert", None, None),
            P("expert", None, None),
            P("expert", None, None),
            P(("groups", "expert"), None),
        ),
        out_specs=P(("groups", "expert"), None),
        check_vma=False,
    )
```

```python
import functools
import math

import jax
import jax.numpy as jnp
from jax import lax
from jax.experimental import pallas as pl
from jax.experimental.pallas import tpu as pltpu
from jax.sharding import PartitionSpec as P

D = 4096
QUERY_HEADS = 32
KEY_VALUE_HEADS = 2
HEAD_SIZE = 128
PAGE_TOKENS = 16
TOPK = 8
MAXB = 16
MAXP = 2


norm_eps = 1e-06
masked_score = -1e30


def partner(x, axis, apart):
    return lax.ppermute(x, axis, [(i, i ^ 1 << apart) for i in range(lax.axis_size(axis))])


def attend(rows_of_queries, rows_of_keys, rows_of_values, allowed, token_own_key, token_own_value):
    decode_tokens = rows_of_queries.shape[0]
    heads_of_queries = rows_of_queries.reshape(
        decode_tokens, KEY_VALUE_HEADS, QUERY_HEADS // KEY_VALUE_HEADS, HEAD_SIZE
    )
    heads_of_keys = rows_of_keys.reshape(decode_tokens, -1, KEY_VALUE_HEADS, HEAD_SIZE)
    heads_of_values = rows_of_values.reshape(decode_tokens, -1, KEY_VALUE_HEADS, HEAD_SIZE)
    scale_for_scores = 1.0 / math.sqrt(HEAD_SIZE)
    allowed_mask = allowed[:, None, None, :]
    scores = (
        jnp.einsum(
            "tkgd,tlkd->tkgl", heads_of_queries, heads_of_keys, preferred_element_type=jnp.float32
        )
        * scale_for_scores
    )
    scores = jnp.where(allowed_mask, scores, masked_score)
    token_own_score = (
        jnp.einsum(
            "xejp,xep->xej",
            heads_of_queries,
            token_own_key.reshape(decode_tokens, KEY_VALUE_HEADS, HEAD_SIZE),
            preferred_element_type=jnp.float32,
        )
        * scale_for_scores
    )
    peak = jnp.maximum(jnp.max(scores, -1), token_own_score)
    weights = jnp.where(allowed_mask, jnp.exp(scores - peak[..., None]), 0.0)
    own_weight = jnp.exp(token_own_score - peak)
    denominator = jnp.sum(weights, -1) + own_weight
    probs = (weights / denominator[..., None]).astype(jnp.bfloat16)
    token_own_probability = (own_weight / denominator).astype(jnp.bfloat16)
    blended_noise = jnp.einsum(
        "tkgl,tlkd->tkgd", probs, heads_of_values, preferred_element_type=jnp.float32
    )
    blended_noise = blended_noise + token_own_probability.astype(jnp.float32)[
        ..., None
    ] * token_own_value.reshape(decode_tokens, KEY_VALUE_HEADS, 1, HEAD_SIZE).astype(jnp.float32)
    return blended_noise.reshape(decode_tokens, QUERY_HEADS * HEAD_SIZE).astype(jnp.bfloat16)


def routed(
    hidden_in,
    queries,
    decode_key_value,
    local_kv,
    page_table,
    seq_blocks,
    prompt_kv,
    prompt_owner,
    prompt_pages,
    norm_gain,
    router,
    w_gate,
    w_up,
    w_down,
    route_ids,
):
    devices = lax.axis_size("expert")
    position = lax.axis_index("expert")
    experts = devices // 2
    seq_dev = hidden_in.shape[0]
    key_value_width = KEY_VALUE_HEADS * HEAD_SIZE
    capacity = min(seq_dev, max(2, 2 * ((3 * seq_dev * TOPK + 2 * devices - 1) // (2 * devices))))
    half_cap = capacity // 2
    even_core = position % 2 == 0
    prompt_count = prompt_owner.shape[0]
    prompt_range = jnp.arange(prompt_count, dtype=jnp.int32)
    same_owner = prompt_owner[:, None] == prompt_owner[None, :]
    earlier = prompt_range[None, :] < prompt_range[:, None]
    arrival = jnp.sum((same_owner & earlier).astype(jnp.int32), 1)
    matching = (
        prompt_owner[None, None, :] == jnp.arange(devices, dtype=jnp.int32)[:, None, None]
    ) & (arrival[None, None, :] == jnp.arange(MAXP, dtype=jnp.int32)[None, :, None])
    chosen_prompt = jnp.sum(jnp.where(matching, prompt_range[None, None, :], 0), -1)
    occupied = jnp.any(matching, -1)
    own_picks = lax.dynamic_index_in_dim(chosen_prompt, position, 0, keepdims=False)
    own_occupied = lax.dynamic_index_in_dim(occupied, position, 0, keepdims=False)
    page_rows = prompt_kv[0]
    outgoing = jnp.take(page_rows, chosen_prompt.T.reshape(-1), axis=0).reshape(
        MAXP, devices, 2, PAGE_TOKENS, key_value_width
    )
    outgoing = jnp.where(occupied.T[:, :, None, None, None], outgoing, 0)
    arrived = lax.all_to_all(outgoing, "expert", split_axis=1, concat_axis=1, tiled=True)
    lengths = jnp.take(prompt_pages, own_picks)
    new_keys = arrived[:, :, 0].reshape(MAXP, devices * PAGE_TOKENS, key_value_width)
    new_values = arrived[:, :, 1].reshape(MAXP, devices * PAGE_TOKENS, key_value_width)
    new_allowed = (jnp.arange(devices * PAGE_TOKENS, dtype=jnp.int32) // PAGE_TOKENS)[
        None, :
    ] < lengths[:, None]
    fresh_rows = attend(
        queries[:MAXP],
        new_keys,
        new_values,
        new_allowed,
        decode_key_value[:MAXP, 0],
        decode_key_value[:MAXP, 1],
    )
    fetched = local_kv[page_table]
    old_keys = fetched[:, :, 0].reshape(seq_dev, MAXB * PAGE_TOKENS, key_value_width)
    old_values = fetched[:, :, 1].reshape(seq_dev, MAXB * PAGE_TOKENS, key_value_width)
    old_allowed = (jnp.arange(MAXB * PAGE_TOKENS, dtype=jnp.int32) // PAGE_TOKENS)[
        None, :
    ] < seq_blocks[:, None]
    old_out = attend(
        queries, old_keys, old_values, old_allowed, decode_key_value[:, 0], decode_key_value[:, 1]
    )
    new_count = jnp.sum(own_occupied.astype(jnp.int32))
    is_new = jnp.arange(MAXP, dtype=jnp.int32) < new_count
    attention = jnp.concatenate(
        [jnp.where(is_new[:, None], fresh_rows, old_out[:MAXP]), old_out[MAXP:]], 0
    )
    residual = (hidden_in.astype(jnp.float32) + attention.astype(jnp.float32)).astype(jnp.bfloat16)
    resid_wide = residual.astype(jnp.float32)
    normed = (
        resid_wide
        * lax.rsqrt(jnp.mean(resid_wide * resid_wide, -1, keepdims=True) + norm_eps)
        * norm_gain
    ).astype(jnp.bfloat16)
    logits = jnp.dot(normed, router, preferred_element_type=jnp.float32)
    expert_onehot = route_ids[:, :, None] == jnp.arange(experts, dtype=jnp.int32)[None, None, :]
    selected = jnp.sum(jnp.where(expert_onehot, logits[:, None, :], 0.0), -1)
    gate_weights = jax.nn.softmax(selected, -1)
    assigned = seq_dev * TOPK
    expert_ids = route_ids.reshape(assigned)
    chosen = (expert_ids[:, None] == jnp.arange(experts, dtype=jnp.int32)[None, :]).astype(
        jnp.int32
    )
    before = jnp.cumsum(chosen, 0) - chosen
    slot_rank = jnp.sum(before * chosen, 1)
    slot_index = expert_ids * capacity + slot_rank
    placing = slot_index[None, :] == jnp.arange(experts * capacity, dtype=jnp.int32)[:, None]
    selector = jnp.any(placing.reshape(experts * capacity, seq_dev, TOPK), -1).astype(jnp.bfloat16)
    gathered_rows = jnp.dot(selector, normed, preferred_element_type=jnp.float32).astype(
        jnp.bfloat16
    )
    outgoing_half = gathered_rows.reshape(devices, half_cap, D)
    own_half = lax.all_to_all(outgoing_half, "expert", split_axis=0, concat_axis=0, tiled=True)
    partner_half = partner(own_half, "expert", 0)
    received = jnp.where(
        even_core,
        jnp.concatenate([own_half, partner_half], 1),
        jnp.concatenate([partner_half, own_half], 1),
    )
    flattened = received.reshape(devices * capacity, D)
    gate_proj = jnp.dot(flattened, w_gate[0], preferred_element_type=jnp.float32)
    up_proj = jnp.dot(flattened, w_up[0], preferred_element_type=jnp.float32)
    activated = (jax.nn.silu(gate_proj) * up_proj).astype(jnp.bfloat16)
    partial_value = jnp.dot(activated, w_down[0], preferred_element_type=jnp.float32).reshape(
        devices, capacity, D
    )
    kept = jnp.where(even_core, partial_value[:, :half_cap], partial_value[:, half_cap:])
    handed = jnp.where(even_core, partial_value[:, half_cap:], partial_value[:, :half_cap])
    partner_part = partner(handed, "expert", 0)
    finished = (kept + partner_part).astype(jnp.bfloat16)
    returned = lax.all_to_all(finished, "expert", split_axis=0, concat_axis=0, tiled=True)
    expert_sum = returned.reshape(experts * capacity, D)
    picked = jnp.take(expert_sum, slot_index, axis=0).astype(jnp.float32).reshape(seq_dev, TOPK, D)
    expert_mix = jnp.sum(picked * gate_weights[:, :, None], 1)
    return (resid_wide + expert_mix).astype(jnp.bfloat16)


def layer_kernel(
    devices,
    owners,
    prompt_lengths,
    blocks,
    pages_hbm,
    q_hbm,
    dkv_hbm,
    table_hbm,
    kv_hbm,
    hidden_hbm,
    gain_hbm,
    router_hbm,
    ids_hbm,
    gate_hbm,
    up_hbm,
    down_hbm,
    out_ref,
    pages_ref,
    q_ref,
    dkv_ref,
    table_ref,
    kv_ref,
    hidden_ref,
    gain_ref,
    router_ref,
    ids_ref,
    w_gate,
    w_up,
    w_down,
    kv_send,
    kv_recv,
    attn,
    x_all,
    gates,
    part,
    core_recv,
    y_send,
    y_recv,
    z_send,
    z_recv,
    kept,
    in_sem,
    w_sem,
    kv_ssem,
    kv_rsem,
    x_ssem,
    x_rsem,
    c_sem,
    y_sem,
    zs_sem,
    zr_sem,
):
    f32, bf16 = jnp.float32, jnp.bfloat16
    me = lax.axis_index("expert")
    lines = devices // 4
    core, row, line = lax.rem(me, 2), lax.rem(me // 2, 2), me // 4
    seqs = hidden_ref.shape[0]
    group = QUERY_HEADS // KEY_VALUE_HEADS
    scale = 1.0 / math.sqrt(HEAD_SIZE)

    def device(at_line, at_row, at_core):
        return (at_line * 2 + at_row) * 2 + at_core

    def place(at_line, at_row, at_core):
        return (at_core * 2 + at_row) * lines + at_line

    def remote(src, dst, ssem, rsem, to):
        return pltpu.make_async_remote_copy(
            src_ref=src,
            dst_ref=dst,
            send_sem=ssem,
            recv_sem=rsem,
            device_id={"expert": to},
            device_id_type=pl.DeviceIdType.MESH,
        )

    loads = [
        pltpu.make_async_copy(a, b, in_sem.at[i])
        for i, (a, b) in enumerate(
            (
                (pages_hbm, pages_ref),
                (q_hbm, q_ref),
                (dkv_hbm, dkv_ref),
                (table_hbm, table_ref),
                (kv_hbm, kv_ref),
                (hidden_hbm, hidden_ref),
                (gain_hbm, gain_ref),
                (router_hbm, router_ref),
                (ids_hbm, ids_ref),
            )
        )
    ]
    weights = [
        pltpu.make_async_copy(a.at[0], b, w_sem.at[i])
        for i, (a, b) in enumerate(((gate_hbm, w_gate), (up_hbm, w_up), (down_hbm, w_down)))
    ]
    for copy in loads + weights:
        copy.start()

    barrier = pltpu.get_barrier_semaphore()

    def greet(k, carry):
        pl.semaphore_signal(
            barrier,
            inc=1,
            device_id={"expert": lax.rem(me + k, devices)},
            device_id_type=pl.DeviceIdType.MESH,
        )
        return carry

    lax.fori_loop(1, devices, greet, 0)

    prompts = owners.shape[0]

    def named(o):
        first, last, number = jnp.int32(0), jnp.int32(0), jnp.int32(0)
        for p in range(prompts):
            hit = owners[p] == o
            last = jnp.where(hit, p, last)
            number = number + hit.astype(jnp.int32)
        for p in reversed(range(prompts)):
            first = jnp.where(owners[p] == o, p, first)
        return (first, last), number

    def stage(o, carry):
        picks, _ = named(o)
        for r in range(MAXP):
            kv_send[o, r] = pages_ref[picks[r]]
        return carry

    loads[0].wait()
    lax.fori_loop(0, devices, stage, 0)
    own_picks, new_count = named(me)
    for r in range(MAXP):
        kv_recv[me, r] = pages_ref[own_picks[r]]
    pl.semaphore_wait(barrier, devices - 1)

    def kv_copy(k):
        to = lax.rem(me + k, devices)
        return remote(kv_send.at[to], kv_recv.at[me], kv_ssem.at[k], kv_rsem.at[k], to)

    def kv_go(k, carry):
        kv_copy(k).start()
        return carry

    lax.fori_loop(1, devices, kv_go, 0)

    for copy in loads[1:]:
        copy.wait()

    def per_seq(values, shape):
        at = lax.broadcasted_iota(jnp.int32, shape, 0)
        return sum(jnp.where(at == s, v, 0) for s, v in enumerate(values))

    tokens = kv_ref.shape[0] * PAGE_TOKENS
    limit = per_seq([blocks[s] for s in range(seqs)], (seqs, tokens))
    page_of = lax.broadcasted_iota(jnp.int32, (seqs, tokens), 1) // PAGE_TOKENS
    held = jnp.zeros((seqs, tokens), f32)
    for b in range(table_ref.shape[1]):
        hit = (page_of == table_ref[:, b : b + 1]) & (limit > b)
        held = held + jnp.where(hit, 1.0, 0.0)
    held = jnp.concatenate([held] * group, 0)

    def heads(h):
        rows = q_ref[...].astype(f32)
        return jnp.concatenate(
            [
                rows[:, (h * group + g) * HEAD_SIZE : (h * group + g + 1) * HEAD_SIZE]
                for g in range(group)
            ],
            0,
        )

    def own(h, at):
        both = dkv_ref[...].astype(f32)
        return jnp.concatenate(
            [both[:, at, h * HEAD_SIZE : (h + 1) * HEAD_SIZE]] * group, 0
        )

    def weigh(scores, times, own_score):
        scores = jnp.where(times > 0, scores, masked_score)
        peak = jnp.maximum(jnp.max(scores, -1, keepdims=True), own_score)
        weight = times * jnp.exp(scores - peak)
        own_weight = jnp.exp(own_score - peak)
        total = jnp.sum(weight, -1, keepdims=True) + own_weight
        return (weight / total).astype(bf16), (own_weight / total).astype(bf16).astype(f32)

    def dot_t(a, b):
        return lax.dot_general(a, b, (((1,), (1,)), ((), ())), preferred_element_type=f32)

    def spread(h, mixed, old):
        for g in range(group):
            at = slice((h * group + g) * HEAD_SIZE, (h * group + g + 1) * HEAD_SIZE)
            rows = mixed[g * seqs : (g + 1) * seqs]
            if old:
                attn[:, at] = rows
            else:
                attn[:, at] = jnp.where(is_new, rows, attn[:, at])

    own_scores = []
    for h in range(KEY_VALUE_HEADS):
        at = slice(h * HEAD_SIZE, (h + 1) * HEAD_SIZE)
        queries = heads(h)
        own_score = jnp.sum(queries * own(h, 0), -1, keepdims=True) * scale
        own_scores.append(own_score)
        keys = kv_ref[:, 0, :, at].reshape(tokens, HEAD_SIZE)
        values = kv_ref[:, 1, :, at].reshape(tokens, HEAD_SIZE)
        probs, own_prob = weigh(dot_t(queries.astype(bf16), keys) * scale, held, own_score)
        mixed = jnp.dot(probs, values, preferred_element_type=f32) + own_prob * own(h, 1)
        spread(h, mixed, True)

    def kv_end(k, carry):
        kv_copy(k).wait()
        return carry

    lax.fori_loop(1, devices, kv_end, 0)

    fresh = devices * PAGE_TOKENS
    slot = lax.rem(lax.broadcasted_iota(jnp.int32, (seqs * group, 1), 0), seqs)
    length = per_seq([prompt_lengths[p] for p in own_picks], (seqs, fresh))
    ahead = lax.broadcasted_iota(jnp.int32, (seqs, fresh), 1) // PAGE_TOKENS < length
    is_new = lax.broadcasted_iota(jnp.int32, (seqs, HEAD_SIZE), 0) < new_count
    allowed = jnp.concatenate([jnp.where(ahead, 1.0, 0.0)] * group, 0)
    for h in range(KEY_VALUE_HEADS):
        at = slice(h * HEAD_SIZE, (h + 1) * HEAD_SIZE)
        queries = heads(h).astype(bf16)
        scores = jnp.zeros((seqs * group, fresh), f32)
        for r in range(MAXP):
            keys = kv_recv[:, r, 0, :, at].reshape(fresh, HEAD_SIZE)
            scores = jnp.where(slot == r, dot_t(queries, keys), scores)
        probs, own_prob = weigh(scores * scale, allowed, own_scores[h])
        mixed = jnp.zeros((seqs * group, HEAD_SIZE), f32)
        for r in range(MAXP):
            values = kv_recv[:, r, 1, :, at].reshape(fresh, HEAD_SIZE)
            mixed = jnp.where(
                slot == r, jnp.dot(probs, values, preferred_element_type=f32), mixed
            )
        spread(h, mixed + own_prob * own(h, 1), False)

    attention = attn[...].astype(bf16).astype(f32)
    wide = (hidden_ref[...].astype(f32) + attention).astype(bf16).astype(f32)
    attn[...] = wide
    mean = jnp.mean(wide * wide, -1, keepdims=True)
    normed = (wide * lax.rsqrt(mean + norm_eps) * gain_ref[...]).astype(bf16)
    mine = place(line, row, core)
    x_all[mine] = normed

    other_row = device(line, 1 - row, core)
    other_core = device(line, row, 1 - core)

    def pass_on(pool, spot, at, to):
        buffer, cols, n, ssem, rsem = pool
        ref = buffer.at[spot, :, cols]
        return remote(ref, ref, ssem.at[n, at], rsem.at[n, spot], to)

    def first_hops(pool):
        copies = [pass_on(pool, mine, 0, other_row)]
        for k in range(1, lines):
            copies.append(pass_on(pool, mine, k, device(lax.rem(line + k, lines), row, core)))
        copies.append(pass_on(pool, mine, lines, other_core))
        for copy in copies:
            copy.start()
        return copies

    def arrived(pool, spot):
        pass_on(pool, spot, 0, other_core).wait_recv()

    pieces = x_rsem.shape[0] - 1
    piece = D // pieces
    pools = [
        (x_all, slice(n * piece, (n + 1) * piece), n, x_ssem, x_rsem) for n in range(pieces)
    ]
    sent = []
    for pool in pools:
        sent += first_hops(pool)

    logits = dot_t(normed, router_ref[...])
    experts = logits.shape[1]
    expert_of = lax.broadcasted_iota(jnp.int32, (seqs, experts), 1)
    times = jnp.zeros((seqs, experts), f32)
    for k in range(ids_ref.shape[1]):
        times = times + jnp.where(ids_ref[:, k : k + 1] == expert_of, 1.0, 0.0)
    picked = jnp.where(times > 0, logits, masked_score)
    gate = times * jnp.exp(picked - jnp.max(picked, -1, keepdims=True))
    gate = gate / jnp.sum(gate, -1, keepdims=True)
    gates[mine] = jnp.concatenate([gate] * (128 // experts), 1)
    pools.append((gates, slice(0, 128), pieces, x_ssem, x_rsem))
    sent += first_hops(pools[-1])

    def over_core(k):
        spot = place(lax.rem(line + k, lines), 1 - row, core)
        for pool in pools:
            arrived(pool, spot)
            copy = pass_on(pool, spot, 3 * lines - 1 + k, other_core)
            copy.start()
            sent.append(copy)

    over_core(0)
    for k in range(1, lines):
        spot = place(lax.rem(line + k, lines), row, core)
        for pool in pools:
            arrived(pool, spot)
            for step, to in ((0, other_row), (1, other_core)):
                copy = pass_on(pool, spot, lines + 2 * k - 1 + step, to)
                copy.start()
                sent.append(copy)
    for k in range(1, lines):
        over_core(k)
    for at_row in range(2):
        for k in range(lines):
            for pool in pools:
                arrived(pool, place(k, at_row, 1 - core))

    weights[0].wait()
    weights[1].wait()
    total = devices * seqs
    hidden = w_gate.shape[1]
    step = min(512, D)

    def project(i, carry):
        at = pl.ds(pl.multiple_of(i * step, step), step)
        x = x_all[:, :, at].reshape(total, step)
        return (
            carry[0] + jnp.dot(x, w_gate[at, :], preferred_element_type=f32),
            carry[1] + jnp.dot(x, w_up[at, :], preferred_element_type=f32),
        )

    zeros = jnp.zeros((total, hidden), f32)
    gate_proj, up_proj = lax.fori_loop(0, D // step, project, (zeros, zeros))
    lanes = lax.broadcasted_iota(jnp.int32, (total, 128), 1)
    scaled = jnp.sum(
        jnp.where(lanes == me // 2, gates[...].reshape(total, 128), 0.0), -1, keepdims=True
    )
    activated = (gate_proj / (1.0 + jnp.exp(-gate_proj)) * up_proj * scaled).astype(bf16)

    weights[2].wait()
    chunks = c_sem.shape[1]
    width = D // chunks

    def cut(i):
        return slice(i * width, (i + 1) * width)

    def core_copy(i):
        return remote(
            part.at[1 - core, :, :, :, cut(i)],
            core_recv.at[:, :, :, cut(i)],
            c_sem.at[0, i],
            c_sem.at[1, i],
            other_core,
        )

    def row_copy(i):
        return remote(
            y_send.at[:, :, cut(i)],
            y_recv.at[:, :, cut(i)],
            y_sem.at[0, i],
            y_sem.at[1, i],
            other_row,
        )

    def line_copy(i, k):
        to = lax.rem(line + k, lines)
        return remote(
            z_send.at[k, :, cut(i)],
            z_recv.at[k, :, cut(i)],
            zs_sem.at[k, i],
            zr_sem.at[k, i],
            device(to, row, core),
        )

    for i in range(chunks):
        rows = jnp.dot(activated, w_down[:, cut(i)], preferred_element_type=f32)
        part[:, :, :, :, cut(i)] = rows.astype(bf16).reshape(2, 2, lines, seqs, width)
        core_copy(i).start()
    for i in range(chunks):
        core_copy(i).wait()
        y_send[:, :, cut(i)] = (
            part[core, 1 - row, :, :, cut(i)].astype(f32)
            + core_recv[1 - row, :, :, cut(i)].astype(f32)
        ).astype(bf16)
        row_copy(i).start()
    for i in range(chunks):
        row_copy(i).wait()

        def summed(at_line):
            return (
                part[core, row, at_line, :, cut(i)].astype(f32)
                + core_recv[row, at_line, :, cut(i)].astype(f32)
                + y_recv[at_line, :, cut(i)].astype(f32)
            )

        for k in range(1, lines):
            z_send[k, :, cut(i)] = summed(lax.rem(line + k, lines)).astype(bf16)
            line_copy(i, k).start()
        kept[:, cut(i)] = attn[:, cut(i)] + summed(line)
    for i in range(chunks):
        answer = kept[:, cut(i)]
        for k in range(1, lines):
            line_copy(i, k).wait()
            answer = answer + z_recv[k, :, cut(i)].astype(f32)
        out_ref[:, cut(i)] = answer.astype(bf16)
    for copy in sent:
        copy.wait_send()


def dense(
    hidden_in,
    queries,
    decode_key_value,
    local_kv,
    page_table,
    seq_blocks,
    prompt_kv,
    prompt_owner,
    prompt_pages,
    norm_gain,
    router,
    w_gate,
    w_up,
    w_down,
    route_ids,
):
    devices = lax.axis_size("expert")
    seqs = hidden_in.shape[0]
    hidden = w_gate.shape[2]
    lines = devices // 4
    bf16, f32 = jnp.bfloat16, jnp.float32
    chunks = 8
    pieces = 2
    loaded = (
        prompt_kv[0],
        queries,
        decode_key_value,
        page_table,
        local_kv,
        hidden_in,
        norm_gain[None, :],
        router.T,
        route_ids,
    )
    smem = pl.BlockSpec(memory_space=pltpu.SMEM)
    vmem = pl.BlockSpec(memory_space=pltpu.VMEM)
    hbm = pl.BlockSpec(memory_space=pltpu.HBM)
    dma = pltpu.SemaphoreType.DMA
    page = (MAXP, 2, PAGE_TOKENS, KEY_VALUE_HEADS * HEAD_SIZE)
    return pl.pallas_call(
        functools.partial(layer_kernel, devices),
        out_shape=jax.ShapeDtypeStruct((seqs, D), bf16),
        in_specs=[smem] * 3 + [hbm] * (len(loaded) + 3),
        out_specs=vmem,
        scratch_shapes=[pltpu.VMEM(a.shape, a.dtype) for a in loaded]
        + [
            pltpu.VMEM((D, hidden), bf16),
            pltpu.VMEM((D, hidden), bf16),
            pltpu.VMEM((hidden, D), bf16),
            pltpu.VMEM((devices,) + page, bf16),
            pltpu.VMEM((devices,) + page, bf16),
            pltpu.VMEM((seqs, D), f32),
            pltpu.VMEM((devices, seqs, D), bf16),
            pltpu.VMEM((devices, seqs, 128), f32),
            pltpu.VMEM((2, 2, lines, seqs, D), bf16),
            pltpu.VMEM((2, lines, seqs, D), bf16),
            pltpu.VMEM((lines, seqs, D), bf16),
            pltpu.VMEM((lines, seqs, D), bf16),
            pltpu.VMEM((lines, seqs, D), bf16),
            pltpu.VMEM((lines, seqs, D), bf16),
            pltpu.VMEM((seqs, D), f32),
            dma((len(loaded),)),
            dma((3,)),
            dma((devices,)),
            dma((devices,)),
            dma((pieces + 1, 4 * lines)),
            dma((pieces + 1, devices)),
            dma((2, chunks)),
            dma((2, chunks)),
            dma((lines, chunks)),
            dma((lines, chunks)),
        ],
        compiler_params=pltpu.CompilerParams(
            collective_id=0, has_side_effects=True, vmem_limit_bytes=67043328
        ),
    )(prompt_owner, prompt_pages, seq_blocks, *loaded, w_gate, w_up, w_down)


def local(*arrays):
    devices = lax.axis_size("expert")
    experts = arrays[10].shape[1]
    if experts == TOPK and devices == 2 * experts and devices % 4 == 0:
        return dense(*arrays)
    return routed(*arrays)


def solution(mesh):
    return jax.shard_map(
        local,
        mesh=mesh,
        in_specs=(
            P(("groups", "expert"), None),
            P(("groups", "expert"), None),
            P(("groups", "expert"), None, None),
            P(("groups", "expert"), None, None, None),
            P(("groups", "expert"), None),
            P(("groups", "expert")),
            P(("groups", "expert"), None, None, None, None),
            P("groups"),
            P("groups"),
            P(),
            P(),
            P("expert", None, None),
            P("expert", None, None),
            P("expert", None, None),
            P(("groups", "expert"), None),
        ),
        out_specs=P(("groups", "expert"), None),
        check_vma=False,
    )
```

```python
import functools
import math

import jax
import jax.numpy as jnp
from jax import lax
from jax.experimental import pallas as pl
from jax.experimental.pallas import tpu as pltpu
from jax.sharding import PartitionSpec as P

D = 4096
QUERY_HEADS = 32
KEY_VALUE_HEADS = 2
HEAD_SIZE = 128
PAGE_TOKENS = 16
TOPK = 8
MAXB = 16
MAXP = 2


norm_eps = 1e-06
masked_score = -1e30


def partner(x, axis, apart):
    return lax.ppermute(x, axis, [(i, i ^ 1 << apart) for i in range(lax.axis_size(axis))])


def attend(rows_of_queries, rows_of_keys, rows_of_values, allowed, token_own_key, token_own_value):
    decode_tokens = rows_of_queries.shape[0]
    heads_of_queries = rows_of_queries.reshape(
        decode_tokens, KEY_VALUE_HEADS, QUERY_HEADS // KEY_VALUE_HEADS, HEAD_SIZE
    )
    heads_of_keys = rows_of_keys.reshape(decode_tokens, -1, KEY_VALUE_HEADS, HEAD_SIZE)
    heads_of_values = rows_of_values.reshape(decode_tokens, -1, KEY_VALUE_HEADS, HEAD_SIZE)
    scale_for_scores = 1.0 / math.sqrt(HEAD_SIZE)
    allowed_mask = allowed[:, None, None, :]
    scores = (
        jnp.einsum(
            "tkgd,tlkd->tkgl", heads_of_queries, heads_of_keys, preferred_element_type=jnp.float32
        )
        * scale_for_scores
    )
    scores = jnp.where(allowed_mask, scores, masked_score)
    token_own_score = (
        jnp.einsum(
            "xejp,xep->xej",
            heads_of_queries,
            token_own_key.reshape(decode_tokens, KEY_VALUE_HEADS, HEAD_SIZE),
            preferred_element_type=jnp.float32,
        )
        * scale_for_scores
    )
    peak = jnp.maximum(jnp.max(scores, -1), token_own_score)
    weights = jnp.where(allowed_mask, jnp.exp(scores - peak[..., None]), 0.0)
    own_weight = jnp.exp(token_own_score - peak)
    denominator = jnp.sum(weights, -1) + own_weight
    probs = (weights / denominator[..., None]).astype(jnp.bfloat16)
    token_own_probability = (own_weight / denominator).astype(jnp.bfloat16)
    blended_noise = jnp.einsum(
        "tkgl,tlkd->tkgd", probs, heads_of_values, preferred_element_type=jnp.float32
    )
    blended_noise = blended_noise + token_own_probability.astype(jnp.float32)[
        ..., None
    ] * token_own_value.reshape(decode_tokens, KEY_VALUE_HEADS, 1, HEAD_SIZE).astype(jnp.float32)
    return blended_noise.reshape(decode_tokens, QUERY_HEADS * HEAD_SIZE).astype(jnp.bfloat16)


def routed(
    hidden_in,
    queries,
    decode_key_value,
    local_kv,
    page_table,
    seq_blocks,
    prompt_kv,
    prompt_owner,
    prompt_pages,
    norm_gain,
    router,
    w_gate,
    w_up,
    w_down,
    route_ids,
):
    devices = lax.axis_size("expert")
    position = lax.axis_index("expert")
    experts = devices // 2
    seq_dev = hidden_in.shape[0]
    key_value_width = KEY_VALUE_HEADS * HEAD_SIZE
    capacity = min(seq_dev, max(2, 2 * ((3 * seq_dev * TOPK + 2 * devices - 1) // (2 * devices))))
    half_cap = capacity // 2
    even_core = position % 2 == 0
    prompt_count = prompt_owner.shape[0]
    prompt_range = jnp.arange(prompt_count, dtype=jnp.int32)
    same_owner = prompt_owner[:, None] == prompt_owner[None, :]
    earlier = prompt_range[None, :] < prompt_range[:, None]
    arrival = jnp.sum((same_owner & earlier).astype(jnp.int32), 1)
    matching = (
        prompt_owner[None, None, :] == jnp.arange(devices, dtype=jnp.int32)[:, None, None]
    ) & (arrival[None, None, :] == jnp.arange(MAXP, dtype=jnp.int32)[None, :, None])
    chosen_prompt = jnp.sum(jnp.where(matching, prompt_range[None, None, :], 0), -1)
    occupied = jnp.any(matching, -1)
    own_picks = lax.dynamic_index_in_dim(chosen_prompt, position, 0, keepdims=False)
    own_occupied = lax.dynamic_index_in_dim(occupied, position, 0, keepdims=False)
    page_rows = prompt_kv[0]
    outgoing = jnp.take(page_rows, chosen_prompt.T.reshape(-1), axis=0).reshape(
        MAXP, devices, 2, PAGE_TOKENS, key_value_width
    )
    outgoing = jnp.where(occupied.T[:, :, None, None, None], outgoing, 0)
    arrived = lax.all_to_all(outgoing, "expert", split_axis=1, concat_axis=1, tiled=True)
    lengths = jnp.take(prompt_pages, own_picks)
    new_keys = arrived[:, :, 0].reshape(MAXP, devices * PAGE_TOKENS, key_value_width)
    new_values = arrived[:, :, 1].reshape(MAXP, devices * PAGE_TOKENS, key_value_width)
    new_allowed = (jnp.arange(devices * PAGE_TOKENS, dtype=jnp.int32) // PAGE_TOKENS)[
        None, :
    ] < lengths[:, None]
    fresh_rows = attend(
        queries[:MAXP],
        new_keys,
        new_values,
        new_allowed,
        decode_key_value[:MAXP, 0],
        decode_key_value[:MAXP, 1],
    )
    fetched = local_kv[page_table]
    old_keys = fetched[:, :, 0].reshape(seq_dev, MAXB * PAGE_TOKENS, key_value_width)
    old_values = fetched[:, :, 1].reshape(seq_dev, MAXB * PAGE_TOKENS, key_value_width)
    old_allowed = (jnp.arange(MAXB * PAGE_TOKENS, dtype=jnp.int32) // PAGE_TOKENS)[
        None, :
    ] < seq_blocks[:, None]
    old_out = attend(
        queries, old_keys, old_values, old_allowed, decode_key_value[:, 0], decode_key_value[:, 1]
    )
    new_count = jnp.sum(own_occupied.astype(jnp.int32))
    is_new = jnp.arange(MAXP, dtype=jnp.int32) < new_count
    attention = jnp.concatenate(
        [jnp.where(is_new[:, None], fresh_rows, old_out[:MAXP]), old_out[MAXP:]], 0
    )
    residual = (hidden_in.astype(jnp.float32) + attention.astype(jnp.float32)).astype(jnp.bfloat16)
    resid_wide = residual.astype(jnp.float32)
    normed = (
        resid_wide
        * lax.rsqrt(jnp.mean(resid_wide * resid_wide, -1, keepdims=True) + norm_eps)
        * norm_gain
    ).astype(jnp.bfloat16)
    logits = jnp.dot(normed, router, preferred_element_type=jnp.float32)
    expert_onehot = route_ids[:, :, None] == jnp.arange(experts, dtype=jnp.int32)[None, None, :]
    selected = jnp.sum(jnp.where(expert_onehot, logits[:, None, :], 0.0), -1)
    gate_weights = jax.nn.softmax(selected, -1)
    assigned = seq_dev * TOPK
    expert_ids = route_ids.reshape(assigned)
    chosen = (expert_ids[:, None] == jnp.arange(experts, dtype=jnp.int32)[None, :]).astype(
        jnp.int32
    )
    before = jnp.cumsum(chosen, 0) - chosen
    slot_rank = jnp.sum(before * chosen, 1)
    slot_index = expert_ids * capacity + slot_rank
    placing = slot_index[None, :] == jnp.arange(experts * capacity, dtype=jnp.int32)[:, None]
    selector = jnp.any(placing.reshape(experts * capacity, seq_dev, TOPK), -1).astype(jnp.bfloat16)
    gathered_rows = jnp.dot(selector, normed, preferred_element_type=jnp.float32).astype(
        jnp.bfloat16
    )
    outgoing_half = gathered_rows.reshape(devices, half_cap, D)
    own_half = lax.all_to_all(outgoing_half, "expert", split_axis=0, concat_axis=0, tiled=True)
    partner_half = partner(own_half, "expert", 0)
    received = jnp.where(
        even_core,
        jnp.concatenate([own_half, partner_half], 1),
        jnp.concatenate([partner_half, own_half], 1),
    )
    flattened = received.reshape(devices * capacity, D)
    gate_proj = jnp.dot(flattened, w_gate[0], preferred_element_type=jnp.float32)
    up_proj = jnp.dot(flattened, w_up[0], preferred_element_type=jnp.float32)
    activated = (jax.nn.silu(gate_proj) * up_proj).astype(jnp.bfloat16)
    partial_value = jnp.dot(activated, w_down[0], preferred_element_type=jnp.float32).reshape(
        devices, capacity, D
    )
    kept = jnp.where(even_core, partial_value[:, :half_cap], partial_value[:, half_cap:])
    handed = jnp.where(even_core, partial_value[:, half_cap:], partial_value[:, :half_cap])
    partner_part = partner(handed, "expert", 0)
    finished = (kept + partner_part).astype(jnp.bfloat16)
    returned = lax.all_to_all(finished, "expert", split_axis=0, concat_axis=0, tiled=True)
    expert_sum = returned.reshape(experts * capacity, D)
    picked = jnp.take(expert_sum, slot_index, axis=0).astype(jnp.float32).reshape(seq_dev, TOPK, D)
    expert_mix = jnp.sum(picked * gate_weights[:, :, None], 1)
    return (resid_wide + expert_mix).astype(jnp.bfloat16)


def layer_kernel(
    devices,
    owners,
    prompt_lengths,
    blocks,
    pages_hbm,
    q_hbm,
    dkv_hbm,
    table_hbm,
    kv_hbm,
    hidden_hbm,
    gain_hbm,
    router_hbm,
    ids_hbm,
    gate_hbm,
    up_hbm,
    down_hbm,
    out_ref,
    pages_ref,
    q_ref,
    dkv_ref,
    table_ref,
    kv_ref,
    hidden_ref,
    gain_ref,
    router_ref,
    ids_ref,
    w_gate,
    w_up,
    w_down,
    kv_send,
    kv_recv,
    attn,
    x_all,
    x_new,
    gates,
    part,
    core_recv,
    y_send,
    y_recv,
    z_send,
    z_recv,
    kept,
    in_sem,
    w_sem,
    kv_ssem,
    kv_rsem,
    x_ssem,
    x_rsem,
    c_sem,
    y_sem,
    zs_sem,
    zr_sem,
):
    f32, bf16 = jnp.float32, jnp.bfloat16
    me = lax.axis_index("expert")
    lines = devices // 4
    core, row, line = lax.rem(me, 2), lax.rem(me // 2, 2), me // 4
    seqs = hidden_ref.shape[0]
    group = QUERY_HEADS // KEY_VALUE_HEADS
    scale = 1.0 / math.sqrt(HEAD_SIZE)

    def device(at_line, at_row, at_core):
        return (at_line * 2 + at_row) * 2 + at_core

    def place(at_line, at_row, at_core):
        return (at_core * 2 + at_row) * lines + at_line

    def remote(src, dst, ssem, rsem, to):
        return pltpu.make_async_remote_copy(
            src_ref=src,
            dst_ref=dst,
            send_sem=ssem,
            recv_sem=rsem,
            device_id={"expert": to},
            device_id_type=pl.DeviceIdType.MESH,
        )

    loads = [
        pltpu.make_async_copy(a, b, in_sem.at[i])
        for i, (a, b) in enumerate(
            (
                (pages_hbm, pages_ref),
                (q_hbm, q_ref),
                (dkv_hbm, dkv_ref),
                (table_hbm, table_ref),
                (kv_hbm, kv_ref),
                (hidden_hbm, hidden_ref),
                (gain_hbm, gain_ref),
                (router_hbm, router_ref),
                (ids_hbm, ids_ref),
            )
        )
    ]
    weights = [
        pltpu.make_async_copy(a.at[0], b, w_sem.at[i])
        for i, (a, b) in enumerate(((gate_hbm, w_gate), (up_hbm, w_up), (down_hbm, w_down)))
    ]
    for copy in loads + weights:
        copy.start()

    barrier = pltpu.get_barrier_semaphore()

    def greet(k, carry):
        pl.semaphore_signal(
            barrier,
            inc=1,
            device_id={"expert": lax.rem(me + k, devices)},
            device_id_type=pl.DeviceIdType.MESH,
        )
        return carry

    lax.fori_loop(1, devices, greet, 0)

    prompts = owners.shape[0]

    def named(o):
        first, last, number = jnp.int32(0), jnp.int32(0), jnp.int32(0)
        for p in range(prompts):
            hit = owners[p] == o
            last = jnp.where(hit, p, last)
            number = number + hit.astype(jnp.int32)
        for p in reversed(range(prompts)):
            first = jnp.where(owners[p] == o, p, first)
        return (first, last), number

    def stage(o, carry):
        picks, _ = named(o)
        for r in range(MAXP):
            kv_send[o, r] = pages_ref[picks[r]]
        return carry

    loads[0].wait()
    lax.fori_loop(0, devices, stage, 0)
    own_picks, new_count = named(me)
    for r in range(MAXP):
        kv_recv[me, r] = pages_ref[own_picks[r]]
    pl.semaphore_wait(barrier, devices - 1)

    def kv_copy(k):
        to = lax.rem(me + k, devices)
        return remote(kv_send.at[to], kv_recv.at[me], kv_ssem.at[k], kv_rsem.at[k], to)

    def kv_go(k, carry):
        kv_copy(k).start()
        return carry

    lax.fori_loop(1, devices, kv_go, 0)

    for copy in loads[1:]:
        copy.wait()

    def per_seq(values, shape):
        at = lax.broadcasted_iota(jnp.int32, shape, 0)
        return sum(jnp.where(at == s, v, 0) for s, v in enumerate(values))

    tokens = kv_ref.shape[0] * PAGE_TOKENS
    limit = per_seq([blocks[s] for s in range(seqs)], (seqs, tokens))
    page_of = lax.broadcasted_iota(jnp.int32, (seqs, tokens), 1) // PAGE_TOKENS
    held = jnp.zeros((seqs, tokens), f32)
    for b in range(table_ref.shape[1]):
        hit = (page_of == table_ref[:, b : b + 1]) & (limit > b)
        held = held + jnp.where(hit, 1.0, 0.0)
    held = jnp.concatenate([held] * group, 0)

    def heads(h):
        rows = q_ref[...].astype(f32)
        return jnp.concatenate(
            [
                rows[:, (h * group + g) * HEAD_SIZE : (h * group + g + 1) * HEAD_SIZE]
                for g in range(group)
            ],
            0,
        )

    def own(h, at):
        both = dkv_ref[...].astype(f32)
        return jnp.concatenate(
            [both[:, at, h * HEAD_SIZE : (h + 1) * HEAD_SIZE]] * group, 0
        )

    def weigh(scores, times, own_score):
        scores = jnp.where(times > 0, scores, masked_score)
        peak = jnp.maximum(jnp.max(scores, -1, keepdims=True), own_score)
        weight = times * jnp.exp(scores - peak)
        own_weight = jnp.exp(own_score - peak)
        total = jnp.sum(weight, -1, keepdims=True) + own_weight
        return (weight / total).astype(bf16), (own_weight / total).astype(bf16).astype(f32)

    def dot_t(a, b):
        return lax.dot_general(a, b, (((1,), (1,)), ((), ())), preferred_element_type=f32)

    def spread(h, mixed, old):
        for g in range(group):
            at = slice((h * group + g) * HEAD_SIZE, (h * group + g + 1) * HEAD_SIZE)
            rows = mixed[g * seqs : (g + 1) * seqs]
            if old:
                attn[:, at] = rows
            else:
                attn[:, at] = jnp.where(is_new, rows, attn[:, at])

    own_scores = []
    for h in range(KEY_VALUE_HEADS):
        at = slice(h * HEAD_SIZE, (h + 1) * HEAD_SIZE)
        queries = heads(h)
        own_score = jnp.sum(queries * own(h, 0), -1, keepdims=True) * scale
        own_scores.append(own_score)
        keys = kv_ref[:, 0, :, at].reshape(tokens, HEAD_SIZE)
        values = kv_ref[:, 1, :, at].reshape(tokens, HEAD_SIZE)
        probs, own_prob = weigh(dot_t(queries.astype(bf16), keys) * scale, held, own_score)
        mixed = jnp.dot(probs, values, preferred_element_type=f32) + own_prob * own(h, 1)
        spread(h, mixed, True)

    def normalize():
        attention = attn[...].astype(bf16).astype(f32)
        wide = (hidden_ref[...].astype(f32) + attention).astype(bf16).astype(f32)
        mean = jnp.mean(wide * wide, -1, keepdims=True)
        return wide, (wide * lax.rsqrt(mean + norm_eps) * gain_ref[...]).astype(bf16)

    mine = place(line, row, core)
    other_row = device(line, 1 - row, core)
    other_core = device(line, row, 1 - core)

    def pass_on(pool, spot, at, to):
        buffer, cols, n, ssem, rsem = pool
        ref = buffer.at[spot, :, cols]
        return remote(ref, ref, ssem.at[n, at], rsem.at[n, spot], to)

    def first_hops(pool):
        copies = [pass_on(pool, mine, 0, other_row)]
        for k in range(1, lines):
            copies.append(pass_on(pool, mine, k, device(lax.rem(line + k, lines), row, core)))
        copies.append(pass_on(pool, mine, lines, other_core))
        for copy in copies:
            copy.start()
        return copies

    def arrived(pool, spot):
        pass_on(pool, spot, 0, other_core).wait_recv()

    pieces = x_rsem.shape[0] - 2
    piece = D // pieces
    pools = [
        (x_all, slice(n * piece, (n + 1) * piece), n, x_ssem, x_rsem) for n in range(pieces)
    ]
    x_all[mine] = normalize()[1]
    sent = []
    for pool in pools:
        sent += first_hops(pool)
    early = tuple(pools)
    pools.append((x_new, slice(0, D), pieces, x_ssem, x_rsem))

    def kv_end(k, carry):
        kv_copy(k).wait()
        return carry

    lax.fori_loop(1, devices, kv_end, 0)

    fresh = devices * PAGE_TOKENS
    slot = lax.rem(lax.broadcasted_iota(jnp.int32, (seqs * group, 1), 0), seqs)
    length = per_seq([prompt_lengths[p] for p in own_picks], (seqs, fresh))
    ahead = lax.broadcasted_iota(jnp.int32, (seqs, fresh), 1) // PAGE_TOKENS < length
    is_new = lax.broadcasted_iota(jnp.int32, (seqs, HEAD_SIZE), 0) < new_count
    allowed = jnp.concatenate([jnp.where(ahead, 1.0, 0.0)] * group, 0)
    for h in range(KEY_VALUE_HEADS):
        at = slice(h * HEAD_SIZE, (h + 1) * HEAD_SIZE)
        queries = heads(h).astype(bf16)
        scores = jnp.zeros((seqs * group, fresh), f32)
        for r in range(MAXP):
            keys = kv_recv[:, r, 0, :, at].reshape(fresh, HEAD_SIZE)
            scores = jnp.where(slot == r, dot_t(queries, keys), scores)
        probs, own_prob = weigh(scores * scale, allowed, own_scores[h])
        mixed = jnp.zeros((seqs * group, HEAD_SIZE), f32)
        for r in range(MAXP):
            values = kv_recv[:, r, 1, :, at].reshape(fresh, HEAD_SIZE)
            mixed = jnp.where(
                slot == r, jnp.dot(probs, values, preferred_element_type=f32), mixed
            )
        spread(h, mixed + own_prob * own(h, 1), False)

    wide, normed = normalize()
    attn[...] = wide
    x_new[mine] = normed[:MAXP]
    sent += first_hops(pools[-1])

    logits = dot_t(normed, router_ref[...])
    experts = logits.shape[1]
    expert_of = lax.broadcasted_iota(jnp.int32, (seqs, experts), 1)
    times = jnp.zeros((seqs, experts), f32)
    for k in range(ids_ref.shape[1]):
        times = times + jnp.where(ids_ref[:, k : k + 1] == expert_of, 1.0, 0.0)
    picked = jnp.where(times > 0, logits, masked_score)
    gate = times * jnp.exp(picked - jnp.max(picked, -1, keepdims=True))
    gate = gate / jnp.sum(gate, -1, keepdims=True)
    gates[mine] = jnp.concatenate([gate] * (128 // experts), 1)
    pools.append((gates, slice(0, 128), pieces + 1, x_ssem, x_rsem))
    sent += first_hops(pools[-1])

    late = tuple(pools[len(early) :])

    def over_row(group_of):
        for k in range(1, lines):
            spot = place(lax.rem(line + k, lines), row, core)
            for pool in group_of:
                arrived(pool, spot)
                for step, to in ((0, other_row), (1, other_core)):
                    copy = pass_on(pool, spot, lines + 2 * k - 1 + step, to)
                    copy.start()
                    sent.append(copy)

    def over_core(group_of):
        for k in range(lines):
            spot = place(lax.rem(line + k, lines), 1 - row, core)
            for pool in group_of:
                arrived(pool, spot)
                copy = pass_on(pool, spot, 3 * lines - 1 + k, other_core)
                copy.start()
                sent.append(copy)

    def settle(group_of):
        for at_row in range(2):
            for k in range(lines):
                for pool in group_of:
                    arrived(pool, place(k, at_row, 1 - core))

    over_row(early)
    over_row(late)
    over_core(early)
    over_core(late)
    settle(early)

    weights[0].wait()
    weights[1].wait()
    total = devices * seqs
    hidden = w_gate.shape[1]
    step = min(512, D)

    def activate(rows, read):
        def project(i, carry):
            at = pl.ds(pl.multiple_of(i * step, step), step)
            x = read(at)
            return (
                carry[0] + jnp.dot(x, w_gate[at, :], preferred_element_type=f32),
                carry[1] + jnp.dot(x, w_up[at, :], preferred_element_type=f32),
            )

        zeros = jnp.zeros((rows, hidden), f32)
        gate_proj, up_proj = lax.fori_loop(0, D // step, project, (zeros, zeros))
        return gate_proj / (1.0 + jnp.exp(-gate_proj)) * up_proj

    wait_rows = activate(total, lambda at: x_all[:, :, at].reshape(total, step))
    settle(late)
    fresh_rows = activate(
        devices * MAXP,
        lambda at: x_new[:, :, at].astype(f32).reshape(devices * MAXP, step).astype(bf16),
    ).astype(bf16)
    token = lax.broadcasted_iota(jnp.int32, (total, devices * MAXP), 0)
    source = lax.broadcasted_iota(jnp.int32, (total, devices * MAXP), 1)
    moved = (token // seqs == source // MAXP) & (lax.rem(token, seqs) == lax.rem(source, MAXP))
    replaced = jnp.dot(
        jnp.where(moved, 1.0, 0.0).astype(bf16), fresh_rows, preferred_element_type=f32
    )
    spot_row = lax.rem(lax.broadcasted_iota(jnp.int32, (total, 1), 0), seqs)
    merged = jnp.where(spot_row < MAXP, replaced, wait_rows)
    lanes = lax.broadcasted_iota(jnp.int32, (total, 128), 1)
    scaled = jnp.sum(
        jnp.where(lanes == me // 2, gates[...].reshape(total, 128), 0.0), -1, keepdims=True
    )
    activated = (merged * scaled).astype(bf16)

    weights[2].wait()
    chunks = c_sem.shape[1]
    width = D // chunks

    def cut(i):
        return slice(i * width, (i + 1) * width)

    def core_copy(i):
        return remote(
            part.at[1 - core, :, :, :, cut(i)],
            core_recv.at[:, :, :, cut(i)],
            c_sem.at[0, i],
            c_sem.at[1, i],
            other_core,
        )

    def row_copy(i):
        return remote(
            y_send.at[:, :, cut(i)],
            y_recv.at[:, :, cut(i)],
            y_sem.at[0, i],
            y_sem.at[1, i],
            other_row,
        )

    def line_copy(i, k):
        to = lax.rem(line + k, lines)
        return remote(
            z_send.at[k, :, cut(i)],
            z_recv.at[k, :, cut(i)],
            zs_sem.at[k, i],
            zr_sem.at[k, i],
            device(to, row, core),
        )

    for i in range(chunks):
        rows = jnp.dot(activated, w_down[:, cut(i)], preferred_element_type=f32)
        part[:, :, :, :, cut(i)] = rows.astype(bf16).reshape(2, 2, lines, seqs, width)
        core_copy(i).start()
    for i in range(chunks):
        core_copy(i).wait()
        y_send[:, :, cut(i)] = (
            part[core, 1 - row, :, :, cut(i)].astype(f32)
            + core_recv[1 - row, :, :, cut(i)].astype(f32)
        ).astype(bf16)
        row_copy(i).start()
    for i in range(chunks):
        row_copy(i).wait()

        def summed(at_line):
            return (
                part[core, row, at_line, :, cut(i)].astype(f32)
                + core_recv[row, at_line, :, cut(i)].astype(f32)
                + y_recv[at_line, :, cut(i)].astype(f32)
            )

        for k in range(1, lines):
            z_send[k, :, cut(i)] = summed(lax.rem(line + k, lines)).astype(bf16)
            line_copy(i, k).start()
        kept[:, cut(i)] = attn[:, cut(i)] + summed(line)
    for i in range(chunks):
        answer = kept[:, cut(i)]
        for k in range(1, lines):
            line_copy(i, k).wait()
            answer = answer + z_recv[k, :, cut(i)].astype(f32)
        out_ref[:, cut(i)] = answer.astype(bf16)
    for copy in sent:
        copy.wait_send()


def dense(
    hidden_in,
    queries,
    decode_key_value,
    local_kv,
    page_table,
    seq_blocks,
    prompt_kv,
    prompt_owner,
    prompt_pages,
    norm_gain,
    router,
    w_gate,
    w_up,
    w_down,
    route_ids,
):
    devices = lax.axis_size("expert")
    seqs = hidden_in.shape[0]
    hidden = w_gate.shape[2]
    lines = devices // 4
    bf16, f32 = jnp.bfloat16, jnp.float32
    chunks = 8
    pieces = 1
    loaded = (
        prompt_kv[0],
        queries,
        decode_key_value,
        page_table,
        local_kv,
        hidden_in,
        norm_gain[None, :],
        router.T,
        route_ids,
    )
    smem = pl.BlockSpec(memory_space=pltpu.SMEM)
    vmem = pl.BlockSpec(memory_space=pltpu.VMEM)
    hbm = pl.BlockSpec(memory_space=pltpu.HBM)
    dma = pltpu.SemaphoreType.DMA
    page = (MAXP, 2, PAGE_TOKENS, KEY_VALUE_HEADS * HEAD_SIZE)
    return pl.pallas_call(
        functools.partial(layer_kernel, devices),
        out_shape=jax.ShapeDtypeStruct((seqs, D), bf16),
        in_specs=[smem] * 3 + [hbm] * (len(loaded) + 3),
        out_specs=vmem,
        scratch_shapes=[pltpu.VMEM(a.shape, a.dtype) for a in loaded]
        + [
            pltpu.VMEM((D, hidden), bf16),
            pltpu.VMEM((D, hidden), bf16),
            pltpu.VMEM((hidden, D), bf16),
            pltpu.VMEM((devices,) + page, bf16),
            pltpu.VMEM((devices,) + page, bf16),
            pltpu.VMEM((seqs, D), f32),
            pltpu.VMEM((devices, seqs, D), bf16),
            pltpu.VMEM((devices, MAXP, D), bf16),
            pltpu.VMEM((devices, seqs, 128), f32),
            pltpu.VMEM((2, 2, lines, seqs, D), bf16),
            pltpu.VMEM((2, lines, seqs, D), bf16),
            pltpu.VMEM((lines, seqs, D), bf16),
            pltpu.VMEM((lines, seqs, D), bf16),
            pltpu.VMEM((lines, seqs, D), bf16),
            pltpu.VMEM((lines, seqs, D), bf16),
            pltpu.VMEM((seqs, D), f32),
            dma((len(loaded),)),
            dma((3,)),
            dma((devices,)),
            dma((devices,)),
            dma((pieces + 2, 4 * lines)),
            dma((pieces + 2, devices)),
            dma((2, chunks)),
            dma((2, chunks)),
            dma((lines, chunks)),
            dma((lines, chunks)),
        ],
        compiler_params=pltpu.CompilerParams(
            collective_id=0, has_side_effects=True, vmem_limit_bytes=67043328
        ),
    )(prompt_owner, prompt_pages, seq_blocks, *loaded, w_gate, w_up, w_down)


def local(*arrays):
    devices = lax.axis_size("expert")
    experts = arrays[10].shape[1]
    if experts == TOPK and devices == 2 * experts and devices % 4 == 0:
        return dense(*arrays)
    return routed(*arrays)


def solution(mesh):
    return jax.shard_map(
        local,
        mesh=mesh,
        in_specs=(
            P(("groups", "expert"), None),
            P(("groups", "expert"), None),
            P(("groups", "expert"), None, None),
            P(("groups", "expert"), None, None, None),
            P(("groups", "expert"), None),
            P(("groups", "expert")),
            P(("groups", "expert"), None, None, None, None),
            P("groups"),
            P("groups"),
            P(),
            P(),
            P("expert", None, None),
            P("expert", None, None),
            P("expert", None, None),
            P(("groups", "expert"), None),
        ),
        out_specs=P(("groups", "expert"), None),
        check_vma=False,
    )
```
